512 devices in a mesh: groups: 2 (over y), fsdp: 16 (over z), mp: 8 (over x), sub: 2 (over core).
Axes of the slice: x: 8, y: 2, z: 16, core: 2. Of those that a mesh axis runs over, the one named last changes fastest.
The devices are a block of a 8x8x16 slice.
Arguments:
- hidden: bfloat16 [512, 36864], P(('groups', 'fsdp', 'sub'), 'mp'), parts along dimension 0, may hold values from -6 to 6
- residual: bfloat16 [512, 4608], P(('groups', 'fsdp', 'sub')), parts along dimension 0, may hold values from -6 to 6
- down_packed: int32 [4608, 4608], P('mp', 'fsdp'), may hold values from -2147483648 to 2147483646
- down_scale: bfloat16 [288, 4608], P('mp', 'fsdp'), may hold values from 0.00049972534 to 0.0019989014
- post_gain: float32 [4608], replicated, may hold values from 0.1 to 1.9
- final_gain: float32 [4608], replicated, may hold values from 0.1 to 1.9
- embed_packed: int32 [131072, 576], P(('fsdp', 'mp', 'sub')), may hold values from -2147483648 to 2147483646
- embed_scale: bfloat16 [131072, 36], P(('fsdp', 'mp', 'sub')), may hold values from 0.0059814453 to 0.029907227
- targets: int32 [512], P(('groups', 'fsdp', 'sub')), parts along dimension 0, may hold values from 0 to 131071
- loss_mask: int32 [512], P(('groups', 'fsdp', 'sub')), parts along dimension 0, may hold values 0 or 1
Outputs:
- token_loss: float32 [512], P(('groups', 'fsdp', 'sub')), parts along dimension 0
- mean_loss: float32 [2], P('groups'), parts along dimension 0
The draws below stay inside these ranges and needn't reach their ends.
There are 2 independent parts, one for each index of `groups`. The reference program is written for one: setup_inputs(seed, part) draws one part's arguments, and reference() takes and returns one part's arrays. A program takes and returns all parts, laid end to end along the dimension named above; an argument that names none is the same for every part. Nothing has to cross between parts.
Inputs may be any that keep to these rules, and one draw needn't show every extreme that they name: `down_packed`: bits 4 k to 4 k + 3 of the word in row r hold the signed code of row 8 r + k of the down projection, k = 0..7. `embed_packed`: bits 4 k to 4 k + 3 of the word in column j hold the signed code of column k * 576 + j of the embedding, k = 0..7.
All inputs are finite; a program needn't handle non-finite values. No bound on the sum of `loss_mask` on one device may be relied on, other than what follows from the above.
Results may differ from the reference program's by a relative error of at most 0.00097.
Values may be sent and summed in bfloat16 or wider, within the bound.
No kernel may reach another device: no remote copies, remote signals or barrier semaphores. Data moves between devices by JAX's collectives and lax.ppermute only.
A program may use at most 64 MiB of HBM per device.

```python
import math
import jax
import jax.numpy as jnp
from jax import lax

D = 4608
FF = 36864
GROUP = 128
VOCAB = 131072
TOKENS = 256
N_MP = 8


def with_ends(entries, stream_key, smallest, largest):
    shape = entries.shape
    spot = [jax.random.randint(jax.random.fold_in(stream_key, axis), (), 0, shape[axis]) for axis in range(len(shape))]
    entries = entries.at[tuple(spot)].set(smallest)
    longest = shape.index(max(shape))
    spot[longest] = (spot[longest] + 1) % shape[longest]
    return entries.at[tuple(spot)].set(largest)


def levels(own_key, extent, pieces, smallest, top_value):
    gain, own = 1.0, jax.random.fold_in(own_key, 6)
    for dim, blocks in pieces:
        steps = jnp.exp(jax.random.uniform(jax.random.fold_in(own, dim), (blocks,), jnp.float32, smallest / len(pieces), top_value / len(pieces)))
        gain = gain * jnp.repeat(steps, extent[dim] // blocks).reshape([-1 if axis == dim else 1 for axis in range(len(extent))])
    return gain


def scatter_about(rng, extent, scale, reach, shards=(), held_as=jnp.bfloat16):
    gain = levels(rng, extent, shards, -0.22, 0.18) if shards else 1.0
    drawn = jax.random.normal(rng, extent, jnp.float32) * scale * gain
    return jnp.minimum(jnp.maximum(drawn, -reach), reach).astype(held_as)


def setup_inputs(seed: int = 0, part: int = 0) -> dict:
    streams_of = jax.random.split(jax.random.key(seed), 11)
    part_keys = jax.random.split(jax.random.fold_in(streams_of[10], part), 11)
    return {
        "hidden": scatter_about(part_keys[0], (TOKENS, FF), 1.0, 6.0, ((0, 32), (1, 8))),
        "residual": scatter_about(part_keys[1], (TOKENS, D), 1.0, 6.0, ((0, 32),)),
        "down_packed": with_ends(jax.random.randint(streams_of[2], (FF // 8, D), -2147483648, 2147483647), jax.random.fold_in(streams_of[2], 1), -2147483648, 2147483646).astype(jnp.int32),
        "down_scale": jnp.clip(jnp.exp(math.log(0.0019989014) - 1.3862944 * jax.random.uniform(streams_of[3], (FF // GROUP, D), jnp.float32) ** levels(streams_of[3], (FF // GROUP, D), ((0, 8), (1, 16)), -0.2, 0.2)), 0.00049972534, 0.0019989014).astype(jnp.bfloat16),
        "post_gain": jnp.clip(1.0 + 0.18 * jax.random.normal(streams_of[4], (D,), jnp.float32), 0.1, 1.9),
        "final_gain": jnp.clip(1.0 + 0.18 * jax.random.normal(streams_of[5], (D,), jnp.float32), 0.1, 1.9),
        "embed_packed": with_ends(jax.random.randint(streams_of[6], (VOCAB, D // 8), -2147483648, 2147483647), jax.random.fold_in(streams_of[6], 1), -2147483648, 2147483646).astype(jnp.int32),
        "embed_scale": jnp.clip(jnp.exp(math.log(0.029907227) - 1.609438 * jax.random.uniform(streams_of[7], (VOCAB, D // GROUP), jnp.float32) ** levels(streams_of[7], (VOCAB, D // GROUP), ((0, 256),), -0.2, 0.2)), 0.0059814453, 0.029907227).astype(jnp.bfloat16),
        "targets": with_ends(jax.random.randint(part_keys[8], (TOKENS,), 0, VOCAB), jax.random.fold_in(part_keys[8], 1), 0, VOCAB - 1).astype(jnp.int32),
        "loss_mask": with_ends((jax.random.randint(part_keys[9], (TOKENS,), 0, 4) < 3).astype(jnp.int32), jax.random.fold_in(part_keys[9], 1), 0, 1),
    }


EPS = 1e-06
CAP = 30.0

def signed_planes(words):
    shifts = (28 - 4 * jnp.arange(8, dtype=jnp.int32))[None, :, None]
    lifted = jnp.left_shift(words[:, None, :], shifts)
    return jnp.right_shift(lifted, 28)

def dequant_down(words, scales):
    cols = words.shape[1]
    codes = signed_planes(words).astype(jnp.bfloat16)
    grouped = codes.reshape(scales.shape[0], -1, cols) * scales[:, None, :]
    return grouped.reshape(-1, cols)

def dequant_embed(words, scales):
    rows = words.shape[0]
    codes = signed_planes(words).astype(jnp.bfloat16)
    grouped = codes.reshape(rows, scales.shape[1], -1) * scales[:, :, None]
    return grouped.reshape(rows, -1)

def reference(hidden, residual, down_packed, down_scale, post_gain, final_gain, embed_packed, embed_scale, targets, loss_mask):
    block = FF // N_MP
    ffn = jnp.zeros((TOKENS, D), jnp.float32)
    for b in range(N_MP):
        weight = dequant_down(down_packed[b * block // 8:(b + 1) * block // 8], down_scale[b * block // GROUP:(b + 1) * block // GROUP])
        ffn = ffn + jnp.dot(hidden[:, b * block:(b + 1) * block], weight, preferred_element_type=jnp.float32)
    normed = ffn * lax.rsqrt(lax.optimization_barrier(jnp.mean(ffn * ffn, axis=-1, keepdims=True)) + EPS) * post_gain
    stream = residual.astype(jnp.float32) + normed
    states = (stream * lax.rsqrt(lax.optimization_barrier(jnp.mean(stream * stream, axis=-1, keepdims=True)) + EPS) * final_gain).astype(jnp.bfloat16)
    vrows = VOCAB // N_MP
    exp_sums = jnp.zeros((TOKENS,), jnp.float32)
    target_logits = jnp.zeros((TOKENS,), jnp.float32)
    for b in range(N_MP):
        embed = dequant_embed(embed_packed[b * vrows:(b + 1) * vrows], embed_scale[b * vrows:(b + 1) * vrows])
        logits = lax.dot_general(states, embed, (((1,), (1,)), ((), ())), preferred_element_type=jnp.float32)
        capped = CAP * jnp.tanh(logits / CAP)
        exp_sums = exp_sums + lax.optimization_barrier(jnp.sum(jnp.exp(capped), axis=1))
        ids = b * vrows + jnp.arange(vrows, dtype=jnp.int32)
        hits = targets[:, None] == ids[None, :]
        target_logits = target_logits + lax.optimization_barrier(jnp.sum(jnp.where(hits, capped, 0.0), axis=1))
    weights = loss_mask.astype(jnp.float32)
    token_loss = weights * (jnp.log(exp_sums) - target_logits)
    mean_loss = jnp.sum(token_loss) / jnp.maximum(jnp.sum(weights), 1.0)
    return (token_loss, mean_loss.reshape(1))
```

```python
import jax
import jax.numpy as jnp
from jax import lax
from jax.sharding import PartitionSpec as P


EPS = 1e-06
CAP = 30.0
GATHER_BYTES = 1 << 20
MXU = 256
LANES = 128


def copy_for_each(value, axis):
    peers = lax.axis_size(axis)
    return lax.all_to_all(
        jnp.broadcast_to(value[None], (peers, *value.shape)), axis, 0, 0, tiled=True
    )


def gather_cut(rows, cols, peers):
    fit = (GATHER_BYTES - 1) // (peers * rows * 2)
    return min(cols, fit // MXU * MXU)


def signed_planes(words):
    shifts = (28 - 4 * jnp.arange(8, dtype=jnp.int32))[None, :, None]
    lifted = jnp.left_shift(words[:, None, :], shifts)
    return jnp.right_shift(lifted, 28)


def dequant_down(words, scales):
    cols = words.shape[1]
    codes = signed_planes(words).astype(jnp.bfloat16)
    grouped = codes.reshape(scales.shape[0], -1, cols) * scales[:, None, :]
    return grouped.reshape(-1, cols)


def dequant_embed(words, scales):
    rows = words.shape[0]
    codes = signed_planes(words).astype(jnp.bfloat16)
    grouped = codes.reshape(rows, scales.shape[1], -1) * scales[:, :, None]
    return grouped.reshape(rows, -1)


def dot_f32(a, b, dims):
    return lax.dot_general(a, b, (dims, ((), ())), preferred_element_type=jnp.float32)


def in_digits(ids):
    return jnp.stack([ids & 255, (ids >> 8) & 255, ids >> 16], axis=-1)


def on_device(
    hidden,
    residual,
    down_packed,
    down_scale,
    post_gain,
    final_gain,
    embed_packed,
    embed_scale,
    targets,
    loss_mask,
):
    toks, width = hidden.shape
    n_z, n_x, n_s = (lax.axis_size(a) for a in ("fsdp", "mp", "sub"))
    z, x, s = (lax.axis_index(a) for a in ("fsdp", "mp", "sub"))
    cols = down_packed.shape[1]
    dim = n_z * cols
    held = n_z * toks
    per_x = held // n_x
    bf16, f32 = jnp.bfloat16, jnp.float32

    cut = gather_cut(toks, width, n_z)
    tail = copy_for_each(hidden[:, cut:], "fsdp").reshape(held, width - cut)
    head = lax.all_gather(hidden[:, :cut], "fsdp").reshape(held, cut)
    group = width // down_scale.shape[0]
    part = dot_f32(
        head, dequant_down(down_packed[: cut // 8], down_scale[: cut // group]), ((1,), (0,))
    ) + dot_f32(tail, dequant_down(down_packed[cut // 8 :], down_scale[cut // group :]), ((1,), (0,)))

    part = jnp.swapaxes(part.reshape(n_z, toks, cols), 0, 1).reshape(n_x, per_x, cols)
    ffn = jnp.sum(lax.all_to_all(part, "mp", 0, 0, tiled=True), axis=0)

    high = lax.reduce_precision(ffn, 8, 7)
    own_row = lax.dynamic_slice_in_dim(residual, x, 1, 0).reshape(n_z, cols)
    own_target = in_digits(lax.dynamic_slice_in_dim(targets, x, 1, 0)).astype(bf16)
    block = jnp.concatenate([high.astype(bf16), (ffn - high).astype(bf16), own_row], axis=0)
    extra = jnp.zeros((block.shape[0], -cols % LANES), bf16)
    extra = lax.dynamic_update_slice(extra, own_target, (2 * per_x, 0))
    block = jnp.concatenate([block, extra], axis=1)
    blocks = lax.all_gather(block, "fsdp")
    rows = (
        blocks[:, :per_x, :cols].astype(f32) + blocks[:, per_x : 2 * per_x, :cols].astype(f32)
    )
    rows = jnp.swapaxes(rows, 0, 1).reshape(per_x, dim)
    res = blocks[:, 2 * per_x :, :cols].astype(f32).reshape(per_x, dim)
    normed = rows * lax.rsqrt(jnp.mean(rows * rows, axis=-1, keepdims=True) + EPS) * post_gain
    stream = res + normed
    states = (
        stream * lax.rsqrt(jnp.mean(stream * stream, axis=-1, keepdims=True) + EPS) * final_gain
    ).astype(bf16)
    digits = jnp.pad(blocks[:, 2 * per_x, cols : cols + 3], ((0, 0), (0, LANES - 3)))

    cut = gather_cut(per_x, dim, n_x)
    tail = jnp.concatenate([states[:, cut:], digits], axis=1)
    tail = jnp.broadcast_to(tail[None], (n_x, *tail.shape))
    head, tail = lax.optimization_barrier((states[:, :cut], tail))
    tail = lax.all_to_all(tail, "mp", 0, 0, tiled=True)
    head = lax.all_gather(head, "mp")
    head = head.reshape(held, cut)
    tail = tail.reshape(held, dim - cut + LANES)
    embed = dequant_embed(embed_packed, embed_scale)
    embed_tail = jnp.pad(embed[:, cut:], ((0, 0), (0, LANES)))
    vocab_rows = embed.shape[0]
    first_id = lax.axis_index(("fsdp", "mp", "sub")) * vocab_rows
    ids = (first_id + jnp.arange(vocab_rows, dtype=jnp.int32))[:, None]
    pick = jnp.array([1.0, 256.0, 65536.0], bf16)
    pick = jnp.pad(pick, (0, LANES - 3))[None, :]

    def sums_of(head, tail):
        logits = dot_f32(embed[:, :cut], head, ((1,), (1,))) + dot_f32(
            embed_tail, tail, ((1,), (1,))
        )
        goal = dot_f32(pick, tail[:, dim - cut :], ((1,), (1,))).astype(jnp.int32)
        capped = CAP * jnp.tanh(logits / CAP)
        return (
            jnp.sum(jnp.exp(capped), axis=0),
            jnp.sum(jnp.where(ids == goal, capped, 0.0), axis=0),
        )

    swap = [(i, n_s - 1 - i) for i in range(n_s)]
    far = (lax.ppermute(head, "sub", swap), lax.ppermute(tail, "sub", swap))
    own_sums, own_goals = sums_of(head, tail)
    far_sums, far_goals = sums_of(*far)

    lane = jnp.arange(held, dtype=jnp.int32)
    spread = jnp.repeat(loss_mask.astype(f32), n_z)
    here = jnp.where((lane % n_z == z) & (x == 0), spread, 0.0)
    own = jnp.stack([own_sums, own_goals, here])
    other = jnp.stack([far_sums, far_goals, jnp.zeros_like(here)])
    packed = jnp.where(s == 0, jnp.concatenate([own, other]), jnp.concatenate([other, own]))
    packed = jnp.sum(copy_for_each(packed, ("mp", "sub")), axis=0)
    packed = jnp.sum(copy_for_each(packed, "fsdp"), axis=0)
    packed = packed.reshape(n_s, 3, held)
    losses = packed[:, 2] * (jnp.log(packed[:, 0]) - packed[:, 1])
    mean_loss = (jnp.sum(losses) / jnp.maximum(jnp.sum(packed[:, 2]), 1.0)).reshape(1)
    mine = jnp.where(s == 0, losses[0], losses[1]).reshape(toks, n_z)
    token_loss = jnp.sum(jnp.where(jnp.arange(n_z) == z, mine, 0.0), axis=1)
    return (token_loss, mean_loss)


def solution(mesh):
    return jax.shard_map(
        on_device,
        mesh=mesh,
        in_specs=(
            P(("groups", "fsdp", "sub"), "mp"),
            P(("groups", "fsdp", "sub"), None),
            P("mp", "fsdp"),
            P("mp", "fsdp"),
            P(),
            P(),
            P(("fsdp", "mp", "sub"), None),
            P(("fsdp", "mp", "sub"), None),
            P(("groups", "fsdp", "sub")),
            P(("groups", "fsdp", "sub")),
        ),
        out_specs=(P(("groups", "fsdp", "sub")), P("groups")),
        check_vma=False,
    )
```

```python
import jax
import jax.numpy as jnp
from jax import lax
from jax.experimental import pallas as pl
from jax.experimental.pallas import tpu as pltpu
from jax.sharding import PartitionSpec as P


EPS = 1e-06
CAP = 30.0
GATHER_BYTES = 1 << 20
MXU = 256
LANES = 128


def copy_for_each(value, axis):
    peers = lax.axis_size(axis)
    return lax.all_to_all(
        jnp.broadcast_to(value[None], (peers, *value.shape)), axis, 0, 0, tiled=True
    )


def gather_cut(rows, cols, peers):
    fit = (GATHER_BYTES - 1) // (peers * rows * 2)
    return min(cols, fit // MXU * MXU)


def signed_planes(words):
    shifts = (28 - 4 * jnp.arange(8, dtype=jnp.int32))[None, :, None]
    lifted = jnp.left_shift(words[:, None, :], shifts)
    return jnp.right_shift(lifted, 28)


def dequant_down(words, scales):
    cols = words.shape[1]
    codes = signed_planes(words).astype(jnp.bfloat16)
    grouped = codes.reshape(scales.shape[0], -1, cols) * scales[:, None, :]
    return grouped.reshape(-1, cols)


def dequant_embed(words, scales):
    rows = words.shape[0]
    codes = signed_planes(words).astype(jnp.bfloat16)
    grouped = codes.reshape(rows, scales.shape[1], -1) * scales[:, :, None]
    return grouped.reshape(rows, -1)


def dot_f32(a, b, dims):
    return lax.dot_general(a, b, (dims, ((), ())), preferred_element_type=jnp.float32)


def in_digits(ids):
    return jnp.stack([ids & 255, (ids >> 8) & 255, ids >> 16], axis=-1)


def split_kernel(hidden_ref, head_ref, tail_ref):
    cut = head_ref.shape[1]
    head_ref[...] = hidden_ref[:, :cut]
    tail_ref[...] = jnp.broadcast_to(hidden_ref[:, cut:][None], tail_ref.shape)


def split_columns(hidden, cut, copies):
    rows, width = hidden.shape
    return pl.pallas_call(
        split_kernel,
        out_shape=(
            jax.ShapeDtypeStruct((rows, cut), hidden.dtype),
            jax.ShapeDtypeStruct((copies, rows, width - cut), hidden.dtype),
        ),
        name="split_columns",
    )(hidden)


def sums_kernel(n_z, pos_ref, mask_ref, head_ref, far_ref, tails_ref, embed_ref, out_ref, st_ref, acc_ref):
    held, cut = head_ref.shape
    blocks, per, _ = tails_ref.shape
    n_s = st_ref.shape[0] // held
    vocab, dim = embed_ref.shape
    step = pl.program_id(0)
    first, s, z, lead = (pos_ref[i] for i in range(4))

    @pl.when(step == 0)
    def _():
        st_ref[pl.ds(pl.multiple_of(s * held, held), held), :cut] = head_ref[...]
        st_ref[pl.ds(pl.multiple_of((n_s - 1 - s) * held, held), held), :cut] = far_ref[...]
        for i in range(blocks):
            row = i % n_s * held + i // n_s * per
            st_ref[row : row + per, cut:] = tails_ref[i]
        acc_ref[...] = jnp.zeros_like(acc_ref)

    logits = dot_f32(embed_ref[...], st_ref[:, :dim], ((1,), (1,)))
    lane = lax.broadcasted_iota(jnp.int32, (8, LANES), 1)
    pick = jnp.where(
        lane == 0, 1.0, jnp.where(lane == 1, 256.0, jnp.where(lane == 2, 65536.0, 0.0))
    )
    goal = dot_f32(pick.astype(jnp.bfloat16), st_ref[:, dim:], ((1,), (1,))).astype(jnp.int32)
    capped = CAP * jnp.tanh(logits / CAP)
    ids = lax.broadcasted_iota(jnp.int32, logits.shape, 0) + (first + step * vocab)
    acc_ref[0:1] += jnp.sum(jnp.exp(capped), axis=0, keepdims=True)
    acc_ref[1:2] += jnp.sum(jnp.where(ids == goal[0:1], capped, 0.0), axis=0, keepdims=True)

    @pl.when(step == pl.num_programs(0) - 1)
    def _():
        place = lax.broadcasted_iota(jnp.int32, (1, n_s * held), 1)
        row = jnp.zeros((1, n_s * held), jnp.float32)
        for i in range(mask_ref.shape[0]):
            row = jnp.where(
                place == s * held + i * n_z + z, (mask_ref[i] * lead).astype(jnp.float32), row
            )
        acc_ref[2:3] = row
        for r in range(3):
            for h in range(n_s):
                part = acc_ref[r : r + 1, h * held : (h + 1) * held]
                out_ref[:, r * n_s + h : r * n_s + h + 1, :] = jnp.broadcast_to(
                    part[None], (out_ref.shape[0], 1, held)
                )


def vocab_sums(pos, mask, head, far, tails, embed, n_z, copies):
    held, _ = head.shape
    vocab, dim = embed.shape
    n_s = tails.shape[0] * tails.shape[1] // held
    step = min(vocab, MXU)
    smem = pl.BlockSpec(memory_space=pltpu.SMEM)
    whole = lambda a: pl.BlockSpec(a.shape, lambda i: (0,) * a.ndim)
    return pl.pallas_call(
        lambda *refs: sums_kernel(n_z, *refs),
        grid=(vocab // step,),
        in_specs=[smem, smem, whole(head), whole(far), whole(tails), pl.BlockSpec((step, dim), lambda i: (i, 0))],
        out_specs=pl.BlockSpec((copies, 3 * n_s, held), lambda i: (0, 0, 0)),
        out_shape=jax.ShapeDtypeStruct((copies, 3 * n_s, held), jnp.float32),
        scratch_shapes=[
            pltpu.VMEM((n_s * held, dim + LANES), jnp.bfloat16),
            pltpu.VMEM((8, n_s * held), jnp.float32),
        ],
        cost_estimate=pl.CostEstimate(
            flops=2 * n_s * held * vocab * dim,
            bytes_accessed=2 * (n_s * held + vocab) * dim,
            transcendentals=2 * n_s * held * vocab,
        ),
        name="vocab_sums",
    )(pos, mask, head, far, tails, embed)


def on_device(
    hidden,
    residual,
    down_packed,
    down_scale,
    post_gain,
    final_gain,
    embed_packed,
    embed_scale,
    targets,
    loss_mask,
):
    toks, width = hidden.shape
    n_z, n_x, n_s = (lax.axis_size(a) for a in ("fsdp", "mp", "sub"))
    z, x, s = (lax.axis_index(a) for a in ("fsdp", "mp", "sub"))
    cols = down_packed.shape[1]
    dim = n_z * cols
    held = n_z * toks
    per_x = held // n_x
    bf16, f32 = jnp.bfloat16, jnp.float32

    cut = gather_cut(toks, width, n_z)
    head, tail = split_columns(hidden, cut, n_z)
    tail = lax.all_to_all(tail, "fsdp", 0, 0, tiled=True)
    head = lax.all_gather(head, "fsdp")
    head, residual, targets, down_packed, down_scale = lax.optimization_barrier(
        (head, residual, targets, down_packed, down_scale)
    )
    weight = dequant_down(down_packed, down_scale)
    part = dot_f32(head.reshape(held, cut), weight[:cut], ((1,), (0,))) + dot_f32(
        tail.reshape(held, width - cut), weight[cut:], ((1,), (0,))
    )

    part = jnp.swapaxes(part.reshape(n_z, toks, cols), 0, 1).reshape(n_x, per_x, cols)
    ffn = jnp.sum(lax.all_to_all(part, "mp", 0, 0, tiled=True), axis=0)

    high = lax.reduce_precision(ffn, 8, 7)
    own_row = lax.dynamic_slice_in_dim(residual, x, 1, 0).reshape(n_z, cols)
    own_target = in_digits(lax.dynamic_slice_in_dim(targets, x, 1, 0)).astype(bf16)
    block = jnp.concatenate([high.astype(bf16), (ffn - high).astype(bf16), own_row], axis=0)
    extra = jnp.zeros((block.shape[0], -cols % LANES), bf16)
    extra = lax.dynamic_update_slice(extra, own_target, (2 * per_x, 0))
    block = jnp.concatenate([block, extra], axis=1)
    blocks = lax.all_gather(block, "fsdp")
    rows = (
        blocks[:, :per_x, :cols].astype(f32) + blocks[:, per_x : 2 * per_x, :cols].astype(f32)
    )
    rows = jnp.swapaxes(rows, 0, 1).reshape(per_x, dim)
    res = blocks[:, 2 * per_x :, :cols].astype(f32).reshape(per_x, dim)
    normed = rows * lax.rsqrt(jnp.mean(rows * rows, axis=-1, keepdims=True) + EPS) * post_gain
    stream = res + normed
    states = (
        stream * lax.rsqrt(jnp.mean(stream * stream, axis=-1, keepdims=True) + EPS) * final_gain
    ).astype(bf16)
    digits = jnp.pad(blocks[:, 2 * per_x, cols : cols + 3], ((0, 0), (0, LANES - 3)))

    cut = gather_cut(per_x, dim, n_x)
    tail = jnp.concatenate([states[:, cut:], digits], axis=1)
    tail = jnp.broadcast_to(tail[None], (n_x * n_s, *tail.shape))
    head, tail = lax.optimization_barrier((states[:, :cut], tail))
    tail = lax.all_to_all(tail, ("mp", "sub"), 0, 0, tiled=True)
    head = lax.all_gather(head, "mp")
    head = head.reshape(held, cut)
    far = lax.ppermute(head, "sub", [(i, n_s - 1 - i) for i in range(n_s)])
    embed = dequant_embed(embed_packed, embed_scale)
    first_id = lax.axis_index(("fsdp", "mp", "sub")) * embed.shape[0]
    pos = jnp.stack([first_id, s, z, (x == 0).astype(jnp.int32)])
    packed = vocab_sums(pos, loss_mask, head, far, tail, embed, n_z, n_x * n_s)

    packed = jnp.sum(lax.all_to_all(packed, ("mp", "sub"), 0, 0, tiled=True), axis=0)
    packed = jnp.sum(copy_for_each(packed, "fsdp"), axis=0)
    sums, goals, mask = packed.reshape(3, n_s, held)
    losses = mask * (jnp.log(sums) - goals)
    mean_loss = (jnp.sum(losses) / jnp.maximum(jnp.sum(mask), 1.0)).reshape(1)
    mine = jnp.where(s == 0, losses[0], losses[1]).reshape(toks, n_z)
    token_loss = jnp.sum(jnp.where(jnp.arange(n_z) == z, mine, 0.0), axis=1)
    return (token_loss, mean_loss)


def solution(mesh):
    return jax.shard_map(
        on_device,
        mesh=mesh,
        in_specs=(
            P(("groups", "fsdp", "sub"), "mp"),
            P(("groups", "fsdp", "sub"), None),
            P("mp", "fsdp"),
            P("mp", "fsdp"),
            P(),
            P(),
            P(("fsdp", "mp", "sub"), None),
            P(("fsdp", "mp", "sub"), None),
            P(("groups", "fsdp", "sub")),
            P(("groups", "fsdp", "sub")),
        ),
        out_specs=(P(("groups", "fsdp", "sub")), P("groups")),
        check_vma=False,
    )
```

```python
import jax
import jax.numpy as jnp
from jax import lax
from jax.experimental import pallas as pl
from jax.experimental.pallas import tpu as pltpu
from jax.sharding import PartitionSpec as P


EPS = 1e-06
CAP = 30.0
GATHER_BYTES = 1 << 20
LANES = 128


def copy_for_each(value, axis):
    peers = lax.axis_size(axis)
    return lax.all_to_all(
        jnp.broadcast_to(value[None], (peers, *value.shape)), axis, 0, 0, tiled=True
    )


def gather_cut(rows, cols, peers):
    fit = (GATHER_BYTES - 1) // (peers * rows * 2)
    return min(cols, fit // LANES * LANES)


def signed_planes(words):
    shifts = (28 - 4 * jnp.arange(8, dtype=jnp.int32))[None, :, None]
    lifted = jnp.left_shift(words[:, None, :], shifts)
    return jnp.right_shift(lifted, 28)


def dequant_down(words, scales):
    cols = words.shape[1]
    codes = signed_planes(words).astype(jnp.bfloat16)
    grouped = codes.reshape(scales.shape[0], -1, cols) * scales[:, None, :]
    return grouped.reshape(-1, cols)


def dequant_embed(words, scales):
    rows = words.shape[0]
    codes = signed_planes(words).astype(jnp.bfloat16)
    grouped = codes.reshape(rows, scales.shape[1], -1) * scales[:, :, None]
    return grouped.reshape(rows, -1)


def dot_f32(a, b, dims):
    return lax.dot_general(a, b, (dims, ((), ())), preferred_element_type=jnp.float32)


def in_digits(ids):
    return jnp.stack([ids & 255, (ids >> 8) & 255, ids >> 16], axis=-1)


def split_kernel(hidden_ref, head_ref, tail_ref):
    cut = head_ref.shape[1]
    head_ref[...] = hidden_ref[:, :cut]
    tail_ref[...] = jnp.broadcast_to(hidden_ref[:, cut:][None], tail_ref.shape)


def split_columns(hidden, cut, copies):
    rows, width = hidden.shape
    return pl.pallas_call(
        split_kernel,
        out_shape=(
            jax.ShapeDtypeStruct((rows, cut), hidden.dtype),
            jax.ShapeDtypeStruct((copies, rows, width - cut), hidden.dtype),
        ),
        name="split_columns",
    )(hidden)


def sums_kernel(n_z, pos_ref, mask_ref, heads, tails, embed_ref, out_ref, st_ref, acc_ref):
    n_s, held, _ = st_ref.shape
    cut = heads[0].shape[1]
    dim, vocab = embed_ref.shape
    first, s, z, lead = (pos_ref[i] for i in range(4))
    for h in range(n_s):
        st_ref[h, :, :cut] = heads[h][...]
        st_ref[h, :, cut:] = tails[h][...]
    states = st_ref.reshape(n_s * held, st_ref.shape[2])
    acc_ref[...] = dot_f32(states[:, :dim], embed_ref[...], ((1,), (0,)))
    digits = states[:, dim:].astype(jnp.float32)
    goal = digits[:, 0:1] + 256.0 * digits[:, 1:2] + 65536.0 * digits[:, 2:3]
    goal = goal.astype(jnp.int32) - first
    sums = jnp.zeros((n_s * held, LANES), jnp.float32)
    hits = jnp.zeros((n_s * held, LANES), jnp.float32)
    for v in range(0, vocab, LANES):
        capped = CAP * jnp.tanh(acc_ref[:, v : v + LANES] / CAP)
        ids = lax.broadcasted_iota(jnp.int32, capped.shape, 1) + v
        sums += jnp.exp(capped)
        hits += jnp.where(ids == goal, capped, 0.0)
    rows = [jnp.sum(r.T, axis=0, keepdims=True) for r in (sums, hits)]
    place = lax.broadcasted_iota(jnp.int32, (1, held), 1)
    mask = jnp.zeros((1, held), jnp.float32)
    for i in range(mask_ref.shape[0]):
        mask = jnp.where(place == i * n_z + z, (mask_ref[i] * lead).astype(jnp.float32), mask)
    rows.append(jnp.concatenate([mask, jnp.zeros_like(mask)], axis=1))
    for r, row in enumerate(rows):
        own, far = row[:, :held], row[:, held:]
        for h in range(n_s):
            part = jnp.where(s == h, own, far)
            out_ref[:, r * n_s + h : r * n_s + h + 1, :] = jnp.broadcast_to(
                part[None], (out_ref.shape[0], 1, held)
            )


def vocab_sums(pos, mask, heads, tails, embed, n_z, copies):
    n_s, (held, cut) = len(heads), heads[0].shape
    dim, vocab = embed.shape
    def kernel(pos_ref, mask_ref, *refs):
        sums_kernel(n_z, pos_ref, mask_ref, refs[:n_s], refs[n_s : 2 * n_s], *refs[2 * n_s :])

    smem = pl.BlockSpec(memory_space=pltpu.SMEM)
    vmem = pl.BlockSpec(memory_space=pltpu.VMEM)
    return pl.pallas_call(
        kernel,
        in_specs=[smem, smem] + [vmem] * (2 * n_s + 1),
        out_shape=jax.ShapeDtypeStruct((copies, 3 * n_s, held), jnp.float32),
        scratch_shapes=[
            pltpu.VMEM((n_s, held, cut + tails[0].shape[1]), jnp.bfloat16),
            pltpu.VMEM((n_s * held, vocab), jnp.float32),
        ],
        compiler_params=pltpu.CompilerParams(vmem_limit_bytes=24 << 20),
        cost_estimate=pl.CostEstimate(
            flops=2 * n_s * held * vocab * dim,
            bytes_accessed=2 * (n_s * held + vocab) * dim,
            transcendentals=2 * n_s * held * vocab,
        ),
        name="vocab_sums",
    )(pos, mask, *heads, *tails, embed)


def on_device(
    hidden,
    residual,
    down_packed,
    down_scale,
    post_gain,
    final_gain,
    embed_packed,
    embed_scale,
    targets,
    loss_mask,
):
    toks, width = hidden.shape
    n_z, n_x, n_s = (lax.axis_size(a) for a in ("fsdp", "mp", "sub"))
    z, x, s = (lax.axis_index(a) for a in ("fsdp", "mp", "sub"))
    cols = down_packed.shape[1]
    dim = n_z * cols
    held = n_z * toks
    per_x = held // n_x
    bf16, f32 = jnp.bfloat16, jnp.float32

    cut = gather_cut(toks, width, n_z)
    head, tail = split_columns(hidden, cut, n_z)
    tail = lax.all_to_all(tail, "fsdp", 0, 0, tiled=True)
    head = lax.all_gather(head, "fsdp")
    head, residual, targets = lax.optimization_barrier((head, residual, targets))
    weight = dequant_down(down_packed, down_scale)
    part = dot_f32(head.reshape(held, cut), weight[:cut], ((1,), (0,))) + dot_f32(
        tail.reshape(held, width - cut), weight[cut:], ((1,), (0,))
    )

    part = jnp.swapaxes(part.reshape(n_z, toks, cols), 0, 1).reshape(n_x, per_x, cols)
    ffn = jnp.sum(lax.all_to_all(part, "mp", 0, 0, tiled=True), axis=0)

    high = lax.reduce_precision(ffn, 8, 7)
    own_row = lax.dynamic_slice_in_dim(residual, x, 1, 0).reshape(n_z, cols)
    own_target = in_digits(lax.dynamic_slice_in_dim(targets, x, 1, 0)).astype(bf16)
    block = jnp.concatenate([high.astype(bf16), (ffn - high).astype(bf16), own_row], axis=0)
    extra = jnp.zeros((block.shape[0], -cols % LANES), bf16)
    extra = lax.dynamic_update_slice(extra, own_target, (2 * per_x, 0))
    block = jnp.concatenate([block, extra], axis=1)
    blocks = lax.all_gather(block, "fsdp")
    rows = (
        blocks[:, :per_x, :cols].astype(f32) + blocks[:, per_x : 2 * per_x, :cols].astype(f32)
    )
    rows = jnp.swapaxes(rows, 0, 1).reshape(per_x, dim)
    res = blocks[:, 2 * per_x :, :cols].astype(f32).reshape(per_x, dim)
    normed = rows * lax.rsqrt(jnp.mean(rows * rows, axis=-1, keepdims=True) + EPS) * post_gain
    stream = res + normed
    states = (
        stream * lax.rsqrt(jnp.mean(stream * stream, axis=-1, keepdims=True) + EPS) * final_gain
    ).astype(bf16)
    digits = jnp.pad(blocks[:, 2 * per_x, cols : cols + 3], ((0, 0), (0, LANES - 3)))

    cut = gather_cut(per_x, dim, n_x)
    tail = jnp.concatenate([states[:, cut:], digits], axis=1)
    tail = jnp.broadcast_to(tail[None], (n_x, *tail.shape))
    head, tail = lax.optimization_barrier((states[:, :cut], tail))
    tail = lax.all_to_all(tail, "mp", 0, 0, tiled=True)
    head = lax.all_gather(head, "mp")
    swap = [(i, n_s - 1 - i) for i in range(n_s)]
    heads = [head.reshape(held, cut)]
    tails = [tail.reshape(held, dim - cut + LANES)]
    tails.append(lax.ppermute(tails[0], "sub", swap))
    heads.append(lax.ppermute(heads[0], "sub", swap))
    embed = dequant_embed(embed_packed, embed_scale)
    first_id = lax.axis_index(("fsdp", "mp", "sub")) * embed.shape[0]
    pos = jnp.stack([first_id, s, z, (x == 0).astype(jnp.int32)])
    packed = vocab_sums(pos, loss_mask, heads, tails, embed.T, n_z, n_x * n_s)

    packed = jnp.sum(lax.all_to_all(packed, ("mp", "sub"), 0, 0, tiled=True), axis=0)
    packed = jnp.sum(copy_for_each(packed, "fsdp"), axis=0)
    sums, goals, mask = packed.reshape(3, n_s, held)
    losses = mask * (jnp.log(sums) - goals)
    mean_loss = (jnp.sum(losses) / jnp.maximum(jnp.sum(mask), 1.0)).reshape(1)
    mine = jnp.where(s == 0, losses[0], losses[1]).reshape(toks, n_z)
    token_loss = jnp.sum(jnp.where(jnp.arange(n_z) == z, mine, 0.0), axis=1)
    return (token_loss, mean_loss)


def solution(mesh):
    return jax.shard_map(
        on_device,
        mesh=mesh,
        in_specs=(
            P(("groups", "fsdp", "sub"), "mp"),
            P(("groups", "fsdp", "sub"), None),
            P("mp", "fsdp"),
            P("mp", "fsdp"),
            P(),
            P(),
            P(("fsdp", "mp", "sub"), None),
            P(("fsdp", "mp", "sub"), None),
            P(("groups", "fsdp", "sub")),
            P(("groups", "fsdp", "sub")),
        ),
        out_specs=(P(("groups", "fsdp", "sub")), P("groups")),
        check_vma=False,
    )
```

```python
import functools

import jax
import jax.numpy as jnp
from jax import lax
from jax.experimental import pallas as pl
from jax.experimental.pallas import tpu as pltpu
from jax.sharding import PartitionSpec as P


EPS = 1e-06
CAP = 30.0
GATHER_BYTES = 1 << 20
LANES = 128
VMEM = pl.BlockSpec(memory_space=pltpu.VMEM)
SMEM = pl.BlockSpec(memory_space=pltpu.SMEM)


def copy_for_each(value, axis):
    peers = lax.axis_size(axis)
    return lax.all_to_all(
        jnp.broadcast_to(value[None], (peers, *value.shape)), axis, 0, 0, tiled=True
    )


def rings(axis):
    n, n_s = lax.axis_size(axis), lax.axis_size("sub")
    return [[i * n_s + (i + r) % n_s for i in range(n)] for r in range(n_s)]


def gather_ring(value, axis):
    return lax.all_gather(value, (axis, "sub"), axis_index_groups=rings(axis))


def exchange_ring(copies, axis):
    return lax.all_to_all(
        copies, (axis, "sub"), 0, 0, tiled=True, axis_index_groups=rings(axis)
    )


def gather_cut(rows, cols, peers):
    fit = (GATHER_BYTES - 1) // (peers * rows * 2)
    return min(cols, fit // LANES * LANES)


def signed_planes(words):
    shifts = (28 - 4 * jnp.arange(8, dtype=jnp.int32))[None, :, None]
    lifted = jnp.left_shift(words[:, None, :], shifts)
    return jnp.right_shift(lifted, 28)


def dequant_down(words, scales):
    cols = words.shape[1]
    codes = signed_planes(words).astype(jnp.bfloat16)
    grouped = codes.reshape(scales.shape[0], -1, cols) * scales[:, None, :]
    return grouped.reshape(-1, cols)


def dequant_embed(words, scales):
    rows = words.shape[0]
    codes = signed_planes(words).astype(jnp.bfloat16)
    grouped = codes.reshape(rows, scales.shape[1], -1) * scales[:, :, None]
    return grouped.reshape(rows, -1)


def dot_f32(a, b, dims):
    return lax.dot_general(a, b, (dims, ((), ())), preferred_element_type=jnp.float32)


def split_kernel(hidden_ref, head_ref, tail_ref):
    cut = head_ref.shape[1]
    head_ref[...] = hidden_ref[:, :cut]
    tail_ref[...] = jnp.broadcast_to(hidden_ref[:, cut:][None], tail_ref.shape)


def split_columns(hidden, cut, copies):
    rows, width = hidden.shape
    return pl.pallas_call(
        split_kernel,
        out_shape=(
            jax.ShapeDtypeStruct((rows, cut), hidden.dtype),
            jax.ShapeDtypeStruct((copies, rows, width - cut), hidden.dtype),
        ),
        in_specs=[VMEM],
        compiler_params=pltpu.CompilerParams(vmem_limit_bytes=4 << 20),
        name="split_columns",
    )(hidden)


def pack_kernel(targets_ref, parts_ref, residual_ref, out_ref):
    per, cols = parts_ref.shape[1:]
    width = out_ref.shape[1]
    ffn = jnp.sum(parts_ref[...], axis=0)
    high = ffn.astype(jnp.bfloat16)
    out_ref[...] = jnp.zeros_like(out_ref)
    out_ref[:per, :cols] = high
    out_ref[per : 2 * per, :cols] = (ffn - high.astype(jnp.float32)).astype(jnp.bfloat16)
    x = lax.axis_index("mp")
    res = residual_ref[...].astype(jnp.float32)
    token = lax.broadcasted_iota(jnp.int32, res.shape, 0)
    res = jnp.sum(jnp.where(token == x, res, 0.0), axis=0, keepdims=True)
    rows = [res[:, c : c + width] for c in range(0, res.shape[1], width)]
    goal = targets_ref[x]
    lane = lax.broadcasted_iota(jnp.int32, (1, width), 1)
    digit = jnp.where(
        lane == 0, goal & 255, jnp.where(lane == 1, (goal >> 8) & 255, jnp.where(lane == 2, goal >> 16, 0))
    )
    rows.append(digit.astype(jnp.float32))
    rows.append(jnp.zeros((out_ref.shape[0] - 2 * per - len(rows), width), jnp.float32))
    out_ref[2 * per :] = jnp.concatenate(rows, axis=0).astype(jnp.bfloat16)


def pack_rows(targets, parts, residual):
    per, cols = parts.shape[1:]
    width = cols + -cols % LANES
    count = 2 * per + residual.shape[1] // width + 1
    return pl.pallas_call(
        pack_kernel,
        in_specs=[SMEM, VMEM, VMEM],
        out_shape=jax.ShapeDtypeStruct((count + -count % 16, width), jnp.bfloat16),
        compiler_params=pltpu.CompilerParams(vmem_limit_bytes=4 << 20),
        name="pack_rows",
    )(targets, parts, residual)


def norm_kernel(blocks_ref, post_ref, final_ref, head_ref, tail_ref, turn_ref):
    n_z = blocks_ref.shape[0]
    per, cut = head_ref.shape
    dim = post_ref.shape[1]
    cols = dim // n_z
    rest, width = turn_ref.shape[1] // n_z, blocks_ref.shape[2]
    f32 = jnp.float32
    ffn = jnp.concatenate(
        [
            blocks_ref[i, :per, :cols].astype(f32) + blocks_ref[i, per : 2 * per, :cols].astype(f32)
            for i in range(n_z)
        ],
        axis=1,
    )
    for i in range(n_z):
        for c in range(width // LANES):
            turn_ref[c, i * rest : (i + 1) * rest] = blocks_ref[
                i, 2 * per :, c * LANES : (c + 1) * LANES
            ].astype(f32)

    def turned(r, c):
        return turn_ref[c, pl.ds(r, n_z, stride=rest), :]

    res = jnp.concatenate(
        [turned(r, c) for r in range(dim // width) for c in range(width // LANES)], axis=1
    )
    scale = lax.rsqrt(jnp.sum(ffn * ffn, axis=1, keepdims=True) / dim + EPS)
    stream = res + ffn * scale * post_ref[...]
    scale = lax.rsqrt(jnp.sum(stream * stream, axis=1, keepdims=True) / dim + EPS)
    states = (stream * scale * final_ref[...]).astype(jnp.bfloat16)
    head_ref[...] = states[:, :cut]
    tail = jnp.concatenate([states[:, cut:], turned(dim // width, 0).astype(jnp.bfloat16)], axis=1)
    tail_ref[...] = jnp.broadcast_to(tail[None], tail_ref.shape)


def norm_rows(blocks, post_gain, final_gain, per, cut, copies):
    n_z, rows, width = blocks.shape
    dim = post_gain.shape[0]
    return pl.pallas_call(
        norm_kernel,
        in_specs=[VMEM] * 3,
        out_shape=(
            jax.ShapeDtypeStruct((per, cut), blocks.dtype),
            jax.ShapeDtypeStruct((copies, per, dim - cut + LANES), blocks.dtype),
        ),
        scratch_shapes=[pltpu.VMEM((width // LANES, n_z * (rows - 2 * per), LANES), jnp.float32)],
        compiler_params=pltpu.CompilerParams(vmem_limit_bytes=8 << 20),
        name="norm_rows",
    )(blocks, post_gain[None], final_gain[None])


def sums_kernel(n_z, mask_ref, heads, tails, embed_ref, out_ref, st_ref, acc_ref):
    n_s, held, _ = st_ref.shape
    cut = heads[0].shape[1]
    dim, vocab = embed_ref.shape
    z, x, s = (lax.axis_index(a) for a in ("fsdp", "mp", "sub"))
    first = ((z * lax.axis_size("mp") + x) * n_s + s) * vocab
    lead = jnp.where(x == 0, 1, 0)
    for h in range(n_s):
        st_ref[h, :, :cut] = heads[h][...]
        st_ref[h, :, cut:] = tails[h][...]
    states = st_ref.reshape(n_s * held, st_ref.shape[2])
    acc_ref[...] = dot_f32(states[:, :dim], embed_ref[...], ((1,), (0,)))
    digits = states[:, dim:].astype(jnp.float32)
    goal = digits[:, 0:1] + 256.0 * digits[:, 1:2] + 65536.0 * digits[:, 2:3]
    goal = goal.astype(jnp.int32) - first
    sums = jnp.zeros((n_s * held, LANES), jnp.float32)
    hits = jnp.zeros((n_s * held, LANES), jnp.float32)
    for v in range(0, vocab, LANES):
        capped = CAP * jnp.tanh(acc_ref[:, v : v + LANES] / CAP)
        ids = lax.broadcasted_iota(jnp.int32, capped.shape, 1) + v
        sums += jnp.exp(capped)
        hits += jnp.where(ids == goal, capped, 0.0)
    rows = [jnp.sum(r.T, axis=0, keepdims=True) for r in (sums, hits)]
    place = lax.broadcasted_iota(jnp.int32, (1, held), 1)
    core = (place + place // n_z + z + x + s) % n_s
    mask = jnp.zeros((1, held), jnp.float32)
    for i in range(mask_ref.shape[0]):
        mask = jnp.where(place == i * n_z + z, (mask_ref[i] * lead).astype(jnp.float32), mask)
    parts = [
        jnp.where(core == h, row[:, :held], row[:, held:]) for row in rows for h in range(n_s)
    ] + [jnp.where(s == h, mask, 0.0) for h in range(n_s)]
    for r, part in enumerate(parts):
        out_ref[:, r : r + 1, :] = jnp.broadcast_to(part[None], (out_ref.shape[0], 1, held))


def vocab_sums(mask, heads, tails, embed, n_z, copies):
    n_s, (held, cut) = len(heads), heads[0].shape
    dim, vocab = embed.shape

    def kernel(mask_ref, *refs):
        sums_kernel(n_z, mask_ref, refs[:n_s], refs[n_s : 2 * n_s], *refs[2 * n_s :])

    return pl.pallas_call(
        kernel,
        in_specs=[SMEM] + [VMEM] * (2 * n_s + 1),
        out_shape=jax.ShapeDtypeStruct((copies, 3 * n_s, held), jnp.float32),
        scratch_shapes=[
            pltpu.VMEM((n_s, held, cut + tails[0].shape[1]), jnp.bfloat16),
            pltpu.VMEM((n_s * held, vocab), jnp.float32),
        ],
        compiler_params=pltpu.CompilerParams(vmem_limit_bytes=24 << 20),
        cost_estimate=pl.CostEstimate(
            flops=2 * n_s * held * vocab * dim,
            bytes_accessed=2 * (n_s * held + vocab) * dim,
            transcendentals=2 * n_s * held * vocab,
        ),
        name="vocab_sums",
    )(mask, *heads, *tails, embed)


def loss_kernel(n_z, packed_ref, token_ref, mean_ref):
    toks = token_ref.shape[0]
    n_s, held = packed_ref.shape[1] // 3, packed_ref.shape[2]
    z, s = lax.axis_index("fsdp"), lax.axis_index("sub")
    packed = jnp.sum(packed_ref[...], axis=0)
    sums, goals, mask = (packed[r * n_s : (r + 1) * n_s] for r in range(3))
    losses = mask * (jnp.log(sums) - goals)
    total, count = jnp.sum(losses), jnp.sum(mask)
    whole = jnp.full((1, held), total) / jnp.maximum(jnp.full((1, held), count), 1.0)
    mean_ref[...] = whole[0, :1]
    core = lax.broadcasted_iota(jnp.int32, losses.shape, 0)
    mine = jnp.sum(jnp.where(core == s, losses, 0.0), axis=0, keepdims=True)
    row = lax.broadcasted_iota(jnp.int32, (held, held), 0)
    lane = lax.broadcasted_iota(jnp.int32, (held, held), 1)
    spread = jnp.where((lane == row * n_z + z) & (row < toks), mine, 0.0)
    token_ref[...] = jnp.sum(spread.T, axis=0)[:toks]


def losses_of(packed, n_z, toks):
    return pl.pallas_call(
        functools.partial(loss_kernel, n_z),
        in_specs=[VMEM],
        out_shape=(
            jax.ShapeDtypeStruct((toks,), jnp.float32),
            jax.ShapeDtypeStruct((1,), jnp.float32),
        ),
        compiler_params=pltpu.CompilerParams(vmem_limit_bytes=4 << 20),
        name="losses_of",
    )(packed)


def on_device(
    hidden,
    residual,
    down_packed,
    down_scale,
    post_gain,
    final_gain,
    embed_packed,
    embed_scale,
    targets,
    loss_mask,
):
    toks, width = hidden.shape
    n_z, n_x, n_s = (lax.axis_size(a) for a in ("fsdp", "mp", "sub"))
    cols = down_packed.shape[1]
    dim = n_z * cols
    held = n_z * toks
    per_x = held // n_x

    cut = gather_cut(toks, width, n_z)
    head, tail = split_columns(hidden, cut, n_z)
    tail = exchange_ring(tail, "fsdp")
    head = gather_ring(head, "fsdp")
    weight = dequant_down(down_packed, down_scale)
    part = dot_f32(head.reshape(held, cut), weight[:cut], ((1,), (0,))) + dot_f32(
        tail.reshape(held, width - cut), weight[cut:], ((1,), (0,))
    )

    part = jnp.swapaxes(part.reshape(n_z, toks, cols), 0, 1).reshape(n_x, per_x, cols)
    parts = lax.all_to_all(part, "mp", 0, 0, tiled=True)
    parts, residual, targets = lax.optimization_barrier((parts, residual, targets))

    block = pack_rows(targets, parts, residual)
    blocks = gather_ring(block, "fsdp")
    blocks, post_gain, final_gain = lax.optimization_barrier((blocks, post_gain, final_gain))

    cut = gather_cut(per_x, dim, n_x)
    head, tail = norm_rows(blocks, post_gain, final_gain, per_x, cut, n_x)
    tail = exchange_ring(tail, "mp")
    head = gather_ring(head, "mp")
    swap = [(i, n_s - 1 - i) for i in range(n_s)]
    heads = [head.reshape(held, cut)]
    tails = [tail.reshape(held, dim - cut + LANES)]
    tails.append(lax.ppermute(tails[0], "sub", swap))
    heads.append(lax.ppermute(heads[0], "sub", swap))
    embed = dequant_embed(embed_packed, embed_scale)
    packed = vocab_sums(loss_mask, heads, tails, embed.T, n_z, n_x * n_s)

    packed = jnp.sum(lax.all_to_all(packed, ("mp", "sub"), 0, 0, tiled=True), axis=0)
    return losses_of(copy_for_each(packed, "fsdp"), n_z, toks)


def solution(mesh):
    return jax.shard_map(
        on_device,
        mesh=mesh,
        in_specs=(
            P(("groups", "fsdp", "sub"), "mp"),
            P(("groups", "fsdp", "sub"), None),
            P("mp", "fsdp"),
            P("mp", "fsdp"),
            P(),
            P(),
            P(("fsdp", "mp", "sub"), None),
            P(("fsdp", "mp", "sub"), None),
            P(("groups", "fsdp", "sub")),
            P(("groups", "fsdp", "sub")),
        ),
        out_specs=(P(("groups", "fsdp", "sub")), P("groups")),
        check_vma=False,
    )
```

```python
import functools

import jax
import jax.numpy as jnp
from jax import lax
from jax.experimental import pallas as pl
from jax.experimental.pallas import tpu as pltpu
from jax.sharding import PartitionSpec as P


EPS = 1e-06
CAP = 30.0
GATHER_BYTES = 1 << 20
LANES = 128
VMEM = pl.BlockSpec(memory_space=pltpu.VMEM)
SMEM = pl.BlockSpec(memory_space=pltpu.SMEM)


def copy_for_each(value, axis):
    peers = lax.axis_size(axis)
    return lax.all_to_all(
        jnp.broadcast_to(value[None], (peers, *value.shape)), axis, 0, 0, tiled=True
    )


def rings(axis):
    n, n_s = lax.axis_size(axis), lax.axis_size("sub")
    return [[i * n_s + (i + r) % n_s for i in range(n)] for r in range(n_s)]


def gather_ring(value, axis):
    return lax.all_gather(value, (axis, "sub"), axis_index_groups=rings(axis))


def exchange_ring(copies, axis):
    return lax.all_to_all(
        copies, (axis, "sub"), 0, 0, tiled=True, axis_index_groups=rings(axis)
    )


def gather_cut(rows, cols, peers):
    fit = (GATHER_BYTES - 1) // (peers * rows * 2)
    return min(cols, fit // LANES * LANES)


def signed_planes(words):
    shifts = (28 - 4 * jnp.arange(8, dtype=jnp.int32))[None, :, None]
    lifted = jnp.left_shift(words[:, None, :], shifts)
    return jnp.right_shift(lifted, 28)


def dequant_down(words, scales):
    cols = words.shape[1]
    codes = signed_planes(words).astype(jnp.bfloat16)
    grouped = codes.reshape(scales.shape[0], -1, cols) * scales[:, None, :]
    return grouped.reshape(-1, cols)


def dequant_embed(words, scales):
    rows = words.shape[0]
    codes = signed_planes(words).astype(jnp.bfloat16)
    grouped = codes.reshape(rows, scales.shape[1], -1) * scales[:, :, None]
    return grouped.reshape(rows, -1)


def dot_f32(a, b, dims):
    return lax.dot_general(a, b, (dims, ((), ())), preferred_element_type=jnp.float32)


def split_kernel(hidden_hbm, words_hbm, head_ref, tail_ref, turned_ref, hidden_ref, words_ref, sem):
    cut = head_ref.shape[1]
    loads = [
        pltpu.make_async_copy(hidden_hbm, hidden_ref, sem.at[0]),
        pltpu.make_async_copy(words_hbm, words_ref, sem.at[1]),
    ]
    for load in loads:
        load.start()
    loads[0].wait()
    head_ref[...] = hidden_ref[:, :cut]
    tail_ref[...] = jnp.broadcast_to(hidden_ref[:, cut:][None], tail_ref.shape)
    loads[1].wait()
    turned_ref[...] = words_ref[...].T


def split_columns(hidden, words, cut, copies):
    rows, width = hidden.shape
    return pl.pallas_call(
        split_kernel,
        in_specs=[pl.BlockSpec(memory_space=pl.ANY)] * 2,
        out_specs=[VMEM] * 3,
        out_shape=(
            jax.ShapeDtypeStruct((rows, cut), hidden.dtype),
            jax.ShapeDtypeStruct((copies, rows, width - cut), hidden.dtype),
            jax.ShapeDtypeStruct(words.shape[::-1], words.dtype),
        ),
        scratch_shapes=[
            pltpu.VMEM(hidden.shape, hidden.dtype),
            pltpu.VMEM(words.shape, words.dtype),
            pltpu.SemaphoreType.DMA((2,)),
        ],
        compiler_params=pltpu.CompilerParams(vmem_limit_bytes=8 << 20),
        name="split_columns",
    )(hidden, words)


def pack_kernel(targets_ref, loss_mask_ref, parts_ref, residual_ref, out_ref):
    per, cols = parts_ref.shape[1:]
    width = out_ref.shape[1]
    ffn = jnp.sum(parts_ref[...], axis=0)
    high = ffn.astype(jnp.bfloat16)
    out_ref[...] = jnp.zeros_like(out_ref)
    out_ref[:per, :cols] = high
    out_ref[per : 2 * per, :cols] = (ffn - high.astype(jnp.float32)).astype(jnp.bfloat16)
    x = lax.axis_index("mp")
    res = residual_ref[...].astype(jnp.float32)
    token = lax.broadcasted_iota(jnp.int32, res.shape, 0)
    res = jnp.sum(jnp.where(token == x, res, 0.0), axis=0, keepdims=True)
    rows = [res[:, c : c + width] for c in range(0, res.shape[1], width)]
    goal = targets_ref[x]
    values = (goal & 255, (goal >> 8) & 255, goal >> 16, loss_mask_ref[x])
    lane = lax.broadcasted_iota(jnp.int32, (1, width), 1)
    digit = jnp.zeros((1, width), jnp.int32)
    for i, value in enumerate(values):
        digit = jnp.where(lane == i, value, digit)
    rows.append(digit.astype(jnp.float32))
    rows.append(jnp.zeros((out_ref.shape[0] - 2 * per - len(rows), width), jnp.float32))
    out_ref[2 * per :] = jnp.concatenate(rows, axis=0).astype(jnp.bfloat16)


def pack_rows(targets, loss_mask, parts, residual):
    per, cols = parts.shape[1:]
    width = cols + -cols % LANES
    count = 2 * per + residual.shape[1] // width + 1
    return pl.pallas_call(
        pack_kernel,
        in_specs=[SMEM, SMEM, VMEM, VMEM],
        out_shape=jax.ShapeDtypeStruct((count + -count % 16, width), jnp.bfloat16),
        compiler_params=pltpu.CompilerParams(vmem_limit_bytes=4 << 20),
        name="pack_rows",
    )(targets, loss_mask, parts, residual)


def norm_kernel(blocks_ref, post_ref, final_ref, head_ref, tail_ref, turn_ref):
    n_z = blocks_ref.shape[0]
    per, cut = head_ref.shape
    dim = post_ref.shape[1]
    cols = dim // n_z
    rest, width = turn_ref.shape[1] // n_z, blocks_ref.shape[2]
    f32 = jnp.float32
    ffn = jnp.concatenate(
        [
            blocks_ref[i, :per, :cols].astype(f32) + blocks_ref[i, per : 2 * per, :cols].astype(f32)
            for i in range(n_z)
        ],
        axis=1,
    )
    for i in range(n_z):
        for c in range(width // LANES):
            turn_ref[c, i * rest : (i + 1) * rest] = blocks_ref[
                i, 2 * per :, c * LANES : (c + 1) * LANES
            ].astype(f32)

    def turned(r, c):
        return turn_ref[c, pl.ds(r, n_z, stride=rest), :]

    res = jnp.concatenate(
        [turned(r, c) for r in range(dim // width) for c in range(width // LANES)], axis=1
    )
    scale = lax.rsqrt(jnp.sum(ffn * ffn, axis=1, keepdims=True) / dim + EPS)
    stream = res + ffn * scale * post_ref[...]
    scale = lax.rsqrt(jnp.sum(stream * stream, axis=1, keepdims=True) / dim + EPS)
    states = (stream * scale * final_ref[...]).astype(jnp.bfloat16)
    head_ref[...] = states[:, :cut]
    tail = jnp.concatenate([states[:, cut:], turned(dim // width, 0).astype(jnp.bfloat16)], axis=1)
    tail_ref[...] = jnp.broadcast_to(tail[None], tail_ref.shape)


def norm_rows(blocks, post_gain, final_gain, per, cut, copies):
    n_z, rows, width = blocks.shape
    dim = post_gain.shape[0]
    return pl.pallas_call(
        norm_kernel,
        in_specs=[VMEM] * 3,
        out_shape=(
            jax.ShapeDtypeStruct((per, cut), blocks.dtype),
            jax.ShapeDtypeStruct((copies, per, dim - cut + LANES), blocks.dtype),
        ),
        scratch_shapes=[pltpu.VMEM((width // LANES, n_z * (rows - 2 * per), LANES), jnp.float32)],
        compiler_params=pltpu.CompilerParams(vmem_limit_bytes=8 << 20),
        name="norm_rows",
    )(blocks, post_gain[None], final_gain[None])


def sums_kernel(n_z, halves, embed_ref, out_ref, mask_ref, st_ref, acc_ref):
    n_s, held, _ = st_ref.shape
    dim, vocab = embed_ref.shape
    z, x, s = (lax.axis_index(a) for a in ("fsdp", "mp", "sub"))
    first = ((z * lax.axis_size("mp") + x) * n_s + s) * vocab
    for h in range(n_s):
        st_ref[h] = halves[h][...]
    states = st_ref.reshape(n_s * held, st_ref.shape[2])
    acc_ref[...] = dot_f32(states[:, :dim], embed_ref[...], ((1,), (0,)))
    digits = states[:, dim:].astype(jnp.float32)
    goal = digits[:, 0:1] + 256.0 * digits[:, 1:2] + 65536.0 * digits[:, 2:3]
    goal = goal.astype(jnp.int32) - first
    sums = jnp.zeros((n_s * held, LANES), jnp.float32)
    hits = jnp.zeros((n_s * held, LANES), jnp.float32)
    for v in range(0, vocab, LANES):
        capped = CAP * jnp.tanh(acc_ref[:, v : v + LANES] / CAP)
        ids = lax.broadcasted_iota(jnp.int32, capped.shape, 1) + v
        sums += jnp.exp(capped)
        hits += jnp.where(ids == goal, capped, 0.0)
    rows = [jnp.sum(r.T, axis=0, keepdims=True) for r in (sums, hits)]
    rows.append(digits.T[3:4])
    place = lax.broadcasted_iota(jnp.int32, (1, held), 1)
    core = (place + place // n_z + z + x + s) % n_s
    parts = [
        jnp.where(core == h, row[:, :held], row[:, held:]) for row in rows for h in range(n_s)
    ]
    mask_ref[...] = jnp.concatenate(parts[2 * n_s :], axis=0)
    part = jnp.concatenate(parts[: 2 * n_s], axis=0)
    out_ref[...] = jnp.broadcast_to(part[None], out_ref.shape)


def vocab_sums(halves, embed, n_z, copies):
    n_s, (held, width) = len(halves), halves[0].shape
    dim, vocab = embed.shape

    def kernel(*refs):
        sums_kernel(n_z, refs[:n_s], *refs[n_s:])

    return pl.pallas_call(
        kernel,
        in_specs=[VMEM] * (n_s + 1),
        out_shape=(
            jax.ShapeDtypeStruct((copies, 2 * n_s, held), jnp.float32),
            jax.ShapeDtypeStruct((n_s, held), jnp.float32),
        ),
        scratch_shapes=[
            pltpu.VMEM((n_s, held, width), jnp.bfloat16),
            pltpu.VMEM((n_s * held, vocab), jnp.float32),
        ],
        compiler_params=pltpu.CompilerParams(vmem_limit_bytes=24 << 20),
        cost_estimate=pl.CostEstimate(
            flops=2 * n_s * held * vocab * dim,
            bytes_accessed=2 * (n_s * held + vocab) * dim,
            transcendentals=2 * n_s * held * vocab,
        ),
        name="vocab_sums",
    )(*halves, embed)


def loss_kernel(n_z, packed_ref, mask_ref, token_ref, mean_ref):
    toks = token_ref.shape[0]
    n_s, held = mask_ref.shape
    z, s = lax.axis_index("fsdp"), lax.axis_index("sub")
    packed = jnp.sum(packed_ref[...], axis=0)
    sums, goals, mask = packed[:n_s], packed[n_s:], mask_ref[...]
    losses = mask * (jnp.log(sums) - goals)
    total, count = jnp.sum(losses), jnp.sum(mask)
    whole = jnp.full((1, held), total) / jnp.maximum(jnp.full((1, held), count), 1.0)
    mean_ref[...] = whole[0, :1]
    core = lax.broadcasted_iota(jnp.int32, losses.shape, 0)
    mine = jnp.sum(jnp.where(core == s, losses, 0.0), axis=0, keepdims=True)
    row = lax.broadcasted_iota(jnp.int32, (held, held), 0)
    lane = lax.broadcasted_iota(jnp.int32, (held, held), 1)
    spread = jnp.where((lane == row * n_z + z) & (row < toks), mine, 0.0)
    token_ref[...] = jnp.sum(spread.T, axis=0)[:toks]


def losses_of(packed, mask, n_z, toks):
    return pl.pallas_call(
        functools.partial(loss_kernel, n_z),
        in_specs=[VMEM, VMEM],
        out_shape=(
            jax.ShapeDtypeStruct((toks,), jnp.float32),
            jax.ShapeDtypeStruct((1,), jnp.float32),
        ),
        compiler_params=pltpu.CompilerParams(vmem_limit_bytes=4 << 20),
        name="losses_of",
    )(packed, mask)


def on_device(
    hidden,
    residual,
    down_packed,
    down_scale,
    post_gain,
    final_gain,
    embed_packed,
    embed_scale,
    targets,
    loss_mask,
):
    toks, width = hidden.shape
    n_z, n_x, n_s = (lax.axis_size(a) for a in ("fsdp", "mp", "sub"))
    cols = down_packed.shape[1]
    dim = n_z * cols
    held = n_z * toks
    per_x = held // n_x

    cut = gather_cut(toks, width, n_z)
    head, tail, down_packed = split_columns(hidden, down_packed.T, cut, n_z)
    tail = exchange_ring(tail, "fsdp")
    head = gather_ring(head, "fsdp")
    weight = dequant_down(down_packed, down_scale)
    part = dot_f32(head.reshape(held, cut), weight[:cut], ((1,), (0,))) + dot_f32(
        tail.reshape(held, width - cut), weight[cut:], ((1,), (0,))
    )

    part = jnp.swapaxes(part.reshape(n_z, toks, cols), 0, 1).reshape(n_x, per_x, cols)
    parts = lax.all_to_all(part, "mp", 0, 0, tiled=True)
    parts, residual, targets = lax.optimization_barrier((parts, residual, targets))

    block = pack_rows(targets, loss_mask, parts, residual)
    blocks = gather_ring(block, "fsdp")
    blocks, post_gain, final_gain = lax.optimization_barrier((blocks, post_gain, final_gain))

    cut = gather_cut(per_x, dim, n_x)
    head, tail = norm_rows(blocks, post_gain, final_gain, per_x, cut, n_x)
    tail = exchange_ring(tail, "mp")
    head = gather_ring(head, "mp")
    own = jnp.concatenate([head.reshape(held, cut), tail.reshape(held, dim - cut + LANES)], axis=1)
    far = lax.ppermute(own, "sub", [(i, n_s - 1 - i) for i in range(n_s)])
    embed = dequant_embed(embed_packed, embed_scale)
    packed, mask = vocab_sums((own, far), embed.T, n_z, n_x * n_s)

    packed = jnp.sum(lax.all_to_all(packed, ("mp", "sub"), 0, 0, tiled=True), axis=0)
    return losses_of(copy_for_each(packed, "fsdp"), mask, n_z, toks)


def solution(mesh):
    return jax.shard_map(
        on_device,
        mesh=mesh,
        in_specs=(
            P(("groups", "fsdp", "sub"), "mp"),
            P(("groups", "fsdp", "sub"), None),
            P("mp", "fsdp"),
            P("mp", "fsdp"),
            P(),
            P(),
            P(("fsdp", "mp", "sub"), None),
            P(("fsdp", "mp", "sub"), None),
            P(("groups", "fsdp", "sub")),
            P(("groups", "fsdp", "sub")),
        ),
        out_specs=(P(("groups", "fsdp", "sub")), P("groups")),
        check_vma=False,
    )
```

```python
import functools

import jax
import jax.numpy as jnp
from jax import lax
from jax.experimental import pallas as pl
from jax.experimental.pallas import tpu as pltpu
from jax.sharding import PartitionSpec as P


EPS = 1e-06
CAP = 30.0
GATHER_BYTES = 1 << 20
LANES = 128
VMEM = pl.BlockSpec(memory_space=pltpu.VMEM)
SMEM = pl.BlockSpec(memory_space=pltpu.SMEM)


def copy_for_each(value, axis):
    peers = lax.axis_size(axis)
    return lax.all_to_all(
        jnp.broadcast_to(value[None], (peers, *value.shape)), axis, 0, 0, tiled=True
    )


def rings(axis):
    n, n_s = lax.axis_size(axis), lax.axis_size("sub")
    return [[i * n_s + (i + r) % n_s for i in range(n)] for r in range(n_s)]


def gather_ring(value, axis):
    return lax.all_gather(value, (axis, "sub"), axis_index_groups=rings(axis))


def exchange_ring(copies, axis):
    return lax.all_to_all(
        copies, (axis, "sub"), 0, 0, tiled=True, axis_index_groups=rings(axis)
    )


def gather_cut(rows, cols, peers):
    fit = (GATHER_BYTES - 1) // (peers * rows * 2)
    return min(cols, fit // LANES * LANES)


def signed_planes(words):
    shifts = (28 - 4 * jnp.arange(8, dtype=jnp.int32))[None, :, None]
    lifted = jnp.left_shift(words[:, None, :], shifts)
    return jnp.right_shift(lifted, 28)


def dequant_down(words, scales):
    cols = words.shape[1]
    codes = signed_planes(words).astype(jnp.bfloat16)
    grouped = codes.reshape(scales.shape[0], -1, cols) * scales[:, None, :]
    return grouped.reshape(-1, cols)


def dequant_embed(words, scales):
    rows = words.shape[0]
    codes = signed_planes(words).astype(jnp.bfloat16)
    grouped = codes.reshape(rows, scales.shape[1], -1) * scales[:, :, None]
    return grouped.reshape(rows, -1)


def dot_f32(a, b, dims):
    return lax.dot_general(a, b, (dims, ((), ())), preferred_element_type=jnp.float32)


def split_kernel(hidden_ref, head_ref, tail_ref):
    cut = head_ref.shape[1]
    head_ref[...] = hidden_ref[:, :cut]
    tail_ref[...] = jnp.broadcast_to(hidden_ref[:, cut:][None], tail_ref.shape)


def split_columns(hidden, cut, copies):
    rows, width = hidden.shape
    return pl.pallas_call(
        split_kernel,
        in_specs=[VMEM],
        out_shape=(
            jax.ShapeDtypeStruct((rows, cut), hidden.dtype),
            jax.ShapeDtypeStruct((copies, rows, width - cut), hidden.dtype),
        ),
        compiler_params=pltpu.CompilerParams(vmem_limit_bytes=4 << 20),
        name="split_columns",
    )(hidden)


def pack_kernel(targets_ref, loss_mask_ref, parts_ref, residual_ref, out_ref):
    per, cols = parts_ref.shape[1:]
    width = out_ref.shape[1]
    ffn = jnp.sum(parts_ref[...], axis=0)
    out_ref[:per] = jnp.zeros((per, width), jnp.bfloat16)
    out_ref[:per, :cols] = ffn.astype(jnp.bfloat16)
    x = lax.axis_index("mp")
    res = residual_ref[...].astype(jnp.float32)
    token = lax.broadcasted_iota(jnp.int32, res.shape, 0)
    res = jnp.sum(jnp.where(token == x, res, 0.0), axis=0, keepdims=True)
    rows = [res[:, c : c + width] for c in range(0, res.shape[1], width)]
    goal = targets_ref[x]
    values = (goal & 255, (goal >> 8) & 255, goal >> 16, loss_mask_ref[x])
    lane = lax.broadcasted_iota(jnp.int32, (1, width), 1)
    digit = jnp.zeros((1, width), jnp.int32)
    for i, value in enumerate(values):
        digit = jnp.where(lane == i, value, digit)
    rows.append(digit.astype(jnp.float32))
    rows.append(jnp.zeros((out_ref.shape[0] - per - len(rows), width), jnp.float32))
    out_ref[per:] = jnp.concatenate(rows, axis=0).astype(jnp.bfloat16)


def pack_rows(targets, loss_mask, parts, residual):
    per, cols = parts.shape[1:]
    width = cols + -cols % LANES
    count = per + residual.shape[1] // width + 1
    return pl.pallas_call(
        pack_kernel,
        in_specs=[SMEM, SMEM, VMEM, VMEM],
        out_shape=jax.ShapeDtypeStruct((count + -count % 16, width), jnp.bfloat16),
        compiler_params=pltpu.CompilerParams(vmem_limit_bytes=4 << 20),
        name="pack_rows",
    )(targets, loss_mask, parts, residual)


def norm_kernel(blocks_ref, post_ref, final_ref, head_ref, tail_ref, turn_ref):
    n_z = blocks_ref.shape[0]
    per, cut = head_ref.shape
    dim = post_ref.shape[1]
    cols = dim // n_z
    rest, width = turn_ref.shape[1] // n_z, blocks_ref.shape[2]
    f32 = jnp.float32
    ffn = jnp.concatenate(
        [blocks_ref[i, :per, :cols].astype(f32) for i in range(n_z)], axis=1
    )
    for i in range(n_z):
        for c in range(width // LANES):
            turn_ref[c, i * rest : (i + 1) * rest] = blocks_ref[
                i, per:, c * LANES : (c + 1) * LANES
            ].astype(f32)

    def turned(r, c):
        return turn_ref[c, pl.ds(r, n_z, stride=rest), :]

    res = jnp.concatenate(
        [turned(r, c) for r in range(dim // width) for c in range(width // LANES)], axis=1
    )
    scale = lax.rsqrt(jnp.sum(ffn * ffn, axis=1, keepdims=True) / dim + EPS)
    stream = res + ffn * scale * post_ref[...]
    scale = lax.rsqrt(jnp.sum(stream * stream, axis=1, keepdims=True) / dim + EPS)
    states = (stream * scale * final_ref[...]).astype(jnp.bfloat16)
    head_ref[...] = states[:, :cut]
    tail = jnp.concatenate([states[:, cut:], turned(dim // width, 0).astype(jnp.bfloat16)], axis=1)
    tail_ref[...] = jnp.broadcast_to(tail[None], tail_ref.shape)


def norm_rows(blocks, post_gain, final_gain, per, cut, copies):
    n_z, rows, width = blocks.shape
    dim = post_gain.shape[0]
    return pl.pallas_call(
        norm_kernel,
        in_specs=[VMEM] * 3,
        out_shape=(
            jax.ShapeDtypeStruct((per, cut), blocks.dtype),
            jax.ShapeDtypeStruct((copies, per, dim - cut + LANES), blocks.dtype),
        ),
        scratch_shapes=[pltpu.VMEM((width // LANES, n_z * (rows - per), LANES), jnp.float32)],
        compiler_params=pltpu.CompilerParams(vmem_limit_bytes=8 << 20),
        name="norm_rows",
    )(blocks, post_gain[None], final_gain[None])


def sums_kernel(n_z, halves, embed_ref, out_ref, mask_ref, st_ref, acc_ref):
    n_s, held, _ = st_ref.shape
    dim, vocab = embed_ref.shape
    z, x, s = (lax.axis_index(a) for a in ("fsdp", "mp", "sub"))
    first = ((z * lax.axis_size("mp") + x) * n_s + s) * vocab
    for h in range(n_s):
        st_ref[h] = halves[h][...]
    states = st_ref.reshape(n_s * held, st_ref.shape[2])
    acc_ref[...] = dot_f32(states[:, :dim], embed_ref[...], ((1,), (0,)))
    digits = states[:, dim:].astype(jnp.float32)
    goal = digits[:, 0:1] + 256.0 * digits[:, 1:2] + 65536.0 * digits[:, 2:3]
    goal = goal.astype(jnp.int32) - first
    sums = jnp.zeros((n_s * held, LANES), jnp.float32)
    hits = jnp.zeros((n_s * held, LANES), jnp.float32)
    for v in range(0, vocab, LANES):
        capped = CAP * jnp.tanh(acc_ref[:, v : v + LANES] / CAP)
        ids = lax.broadcasted_iota(jnp.int32, capped.shape, 1) + v
        sums += jnp.exp(capped)
        hits += jnp.where(ids == goal, capped, 0.0)
    rows = [jnp.sum(r.T, axis=0, keepdims=True) for r in (sums, hits)]
    rows.append(digits.T[3:4])
    place = lax.broadcasted_iota(jnp.int32, (1, held), 1)
    core = (place + place // n_z + z + x + s) % n_s
    parts = [
        jnp.where(core == h, row[:, :held], row[:, held:]) for row in rows for h in range(n_s)
    ]
    mask_ref[...] = jnp.concatenate(parts[2 * n_s :], axis=0)
    part = jnp.concatenate(parts[: 2 * n_s], axis=0)
    out_ref[...] = jnp.broadcast_to(part[None], out_ref.shape)


def vocab_sums(halves, embed, n_z, copies):
    n_s, (held, width) = len(halves), halves[0].shape
    dim, vocab = embed.shape

    def kernel(*refs):
        sums_kernel(n_z, refs[:n_s], *refs[n_s:])

    return pl.pallas_call(
        kernel,
        in_specs=[VMEM] * (n_s + 1),
        out_shape=(
            jax.ShapeDtypeStruct((copies, 2 * n_s, held), jnp.float32),
            jax.ShapeDtypeStruct((n_s, held), jnp.float32),
        ),
        scratch_shapes=[
            pltpu.VMEM((n_s, held, width), jnp.bfloat16),
            pltpu.VMEM((n_s * held, vocab), jnp.float32),
        ],
        compiler_params=pltpu.CompilerParams(vmem_limit_bytes=24 << 20),
        cost_estimate=pl.CostEstimate(
            flops=2 * n_s * held * vocab * dim,
            bytes_accessed=2 * (n_s * held + vocab) * dim,
            transcendentals=2 * n_s * held * vocab,
        ),
        name="vocab_sums",
    )(*halves, embed)


def loss_kernel(n_z, packed_ref, mask_ref, token_ref, mean_ref):
    toks = token_ref.shape[0]
    n_s, held = mask_ref.shape
    z, s = lax.axis_index("fsdp"), lax.axis_index("sub")
    packed = jnp.sum(packed_ref[...], axis=0)
    sums, goals, mask = packed[:n_s], packed[n_s:], mask_ref[...]
    losses = mask * (jnp.log(sums) - goals)
    total, count = jnp.sum(losses), jnp.sum(mask)
    whole = jnp.full((1, held), total) / jnp.maximum(jnp.full((1, held), count), 1.0)
    mean_ref[...] = whole[0, :1]
    core = lax.broadcasted_iota(jnp.int32, losses.shape, 0)
    mine = jnp.sum(jnp.where(core == s, losses, 0.0), axis=0, keepdims=True)
    row = lax.broadcasted_iota(jnp.int32, (held, held), 0)
    lane = lax.broadcasted_iota(jnp.int32, (held, held), 1)
    spread = jnp.where((lane == row * n_z + z) & (row < toks), mine, 0.0)
    token_ref[...] = jnp.sum(spread.T, axis=0)[:toks]


def losses_of(packed, mask, n_z, toks):
    return pl.pallas_call(
        functools.partial(loss_kernel, n_z),
        in_specs=[VMEM, VMEM],
        out_shape=(
            jax.ShapeDtypeStruct((toks,), jnp.float32),
            jax.ShapeDtypeStruct((1,), jnp.float32),
        ),
        compiler_params=pltpu.CompilerParams(vmem_limit_bytes=4 << 20),
        name="losses_of",
    )(packed, mask)


def on_device(
    hidden,
    residual,
    down_packed,
    down_scale,
    post_gain,
    final_gain,
    embed_packed,
    embed_scale,
    targets,
    loss_mask,
):
    toks, width = hidden.shape
    n_z, n_x, n_s = (lax.axis_size(a) for a in ("fsdp", "mp", "sub"))
    cols = down_packed.shape[1]
    dim = n_z * cols
    held = n_z * toks
    per_x = held // n_x

    cut = gather_cut(toks, width, n_z)
    head, tail = split_columns(hidden, cut, n_z)
    tail = exchange_ring(tail, "fsdp")
    head = gather_ring(head, "fsdp")
    weight = dequant_down(down_packed, down_scale)
    part = dot_f32(head.reshape(held, cut), weight[:cut], ((1,), (0,))) + dot_f32(
        tail.reshape(held, width - cut), weight[cut:], ((1,), (0,))
    )

    part = jnp.swapaxes(part.reshape(n_z, toks, cols), 0, 1).reshape(n_x, per_x, cols)
    parts = lax.all_to_all(part, "mp", 0, 0, tiled=True)
    parts, residual, targets = lax.optimization_barrier((parts, residual, targets))

    block = pack_rows(targets, loss_mask, parts, residual)
    blocks = gather_ring(block, "fsdp")
    blocks, post_gain, final_gain = lax.optimization_barrier((blocks, post_gain, final_gain))

    cut = gather_cut(per_x, dim, n_x)
    head, tail = norm_rows(blocks, post_gain, final_gain, per_x, cut, n_x)
    tail = exchange_ring(tail, "mp")
    head = gather_ring(head, "mp")
    own = jnp.concatenate([head.reshape(held, cut), tail.reshape(held, dim - cut + LANES)], axis=1)
    far = lax.ppermute(own, "sub", [(i, n_s - 1 - i) for i in range(n_s)])
    embed = dequant_embed(embed_packed, embed_scale)
    packed, mask = vocab_sums((own, far), embed.T, n_z, n_x * n_s)

    packed = jnp.sum(lax.all_to_all(packed, ("mp", "sub"), 0, 0, tiled=True), axis=0)
    return losses_of(copy_for_each(packed, "fsdp"), mask, n_z, toks)


def solution(mesh):
    return jax.shard_map(
        on_device,
        mesh=mesh,
        in_specs=(
            P(("groups", "fsdp", "sub"), "mp"),
            P(("groups", "fsdp", "sub"), None),
            P("mp", "fsdp"),
            P("mp", "fsdp"),
            P(),
            P(),
            P(("fsdp", "mp", "sub"), None),
            P(("fsdp", "mp", "sub"), None),
            P(("groups", "fsdp", "sub")),
            P(("groups", "fsdp", "sub")),
        ),
        out_specs=(P(("groups", "fsdp", "sub")), P("groups")),
        check_vma=False,
    )
```

```python
import functools

import jax
import jax.numpy as jnp
from jax import lax
from jax.experimental import pallas as pl
from jax.experimental.pallas import tpu as pltpu
from jax.sharding import PartitionSpec as P


EPS = 1e-06
CAP = 30.0
GATHER_BYTES = 1 << 20
LANES = 128
VMEM = pl.BlockSpec(memory_space=pltpu.VMEM)
SMEM = pl.BlockSpec(memory_space=pltpu.SMEM)


def copy_for_each(value, axis):
    peers = lax.axis_size(axis)
    return lax.all_to_all(
        jnp.broadcast_to(value[None], (peers, *value.shape)), axis, 0, 0, tiled=True
    )


def rings(axis):
    n, n_s = lax.axis_size(axis), lax.axis_size("sub")
    return [[i * n_s + (i + r) % n_s for i in range(n)] for r in range(n_s)]


def gather_ring(value, axis):
    return lax.all_gather(value, (axis, "sub"), axis_index_groups=rings(axis))


def exchange_ring(copies, axis):
    return lax.all_to_all(
        copies, (axis, "sub"), 0, 0, tiled=True, axis_index_groups=rings(axis)
    )


def gather_cut(rows, cols, peers):
    fit = (GATHER_BYTES - 1) // (peers * rows * 2)
    return min(cols, fit // LANES * LANES)


def signed_planes(words):
    shifts = (28 - 4 * jnp.arange(8, dtype=jnp.int32))[None, :, None]
    lifted = jnp.left_shift(words[:, None, :], shifts)
    return jnp.right_shift(lifted, 28)


def dequant_down(words, scales):
    cols = words.shape[1]
    codes = signed_planes(words).astype(jnp.bfloat16)
    grouped = codes.reshape(scales.shape[0], -1, cols) * scales[:, None, :]
    return grouped.reshape(-1, cols)


def dequant_embed(words, scales):
    rows = words.shape[0]
    codes = signed_planes(words).astype(jnp.bfloat16)
    grouped = codes.reshape(rows, scales.shape[1], -1) * scales[:, :, None]
    return grouped.reshape(rows, -1)


def dot_f32(a, b, dims):
    return lax.dot_general(a, b, (dims, ((), ())), preferred_element_type=jnp.float32)


def split_kernel(hidden_ref, head_ref, tail_ref):
    cut = head_ref.shape[1]
    head_ref[...] = hidden_ref[:, :cut]
    tail_ref[...] = jnp.broadcast_to(hidden_ref[:, cut:][None], tail_ref.shape)


def split_columns(hidden, cut, copies):
    rows, width = hidden.shape
    return pl.pallas_call(
        split_kernel,
        in_specs=[VMEM],
        out_shape=(
            jax.ShapeDtypeStruct((rows, cut), hidden.dtype),
            jax.ShapeDtypeStruct((copies, rows, width - cut), hidden.dtype),
        ),
        compiler_params=pltpu.CompilerParams(vmem_limit_bytes=4 << 20),
        name="split_columns",
    )(hidden)


def pack_kernel(targets_ref, loss_mask_ref, parts_ref, residual_ref, out_ref):
    per, cols = parts_ref.shape[1:]
    width = out_ref.shape[1]
    ffn = jnp.sum(parts_ref[...], axis=0)
    high = ffn.astype(jnp.bfloat16)
    low = (ffn - high.astype(jnp.float32)).astype(jnp.bfloat16)
    out_ref[:per, :cols] = high
    out_ref[:per, cols:] = low[:, : width - cols]
    x = lax.axis_index("mp")
    res = residual_ref[...].astype(jnp.float32)
    token = lax.broadcasted_iota(jnp.int32, res.shape, 0)
    res = jnp.sum(jnp.where(token == x, res, 0.0), axis=0, keepdims=True)
    rows = [res[:, c : c + width] for c in range(0, res.shape[1], width)]
    goal = targets_ref[x]
    values = (goal & 255, (goal >> 8) & 255, goal >> 16, loss_mask_ref[x])
    lane = lax.broadcasted_iota(jnp.int32, (1, width), 1)
    digit = jnp.zeros((1, width), jnp.int32)
    for i, value in enumerate(values):
        digit = jnp.where(lane == i, value, digit)
    rows.append(digit.astype(jnp.float32))
    rows.append(jnp.zeros((out_ref.shape[0] - per - len(rows), width), jnp.float32))
    out_ref[per:] = jnp.concatenate(rows, axis=0).astype(jnp.bfloat16)


def pack_rows(targets, loss_mask, parts, residual):
    per, cols = parts.shape[1:]
    width = cols + -cols % LANES
    count = per + residual.shape[1] // width + 1
    return pl.pallas_call(
        pack_kernel,
        in_specs=[SMEM, SMEM, VMEM, VMEM],
        out_shape=jax.ShapeDtypeStruct((count + -count % 16, width), jnp.bfloat16),
        compiler_params=pltpu.CompilerParams(vmem_limit_bytes=4 << 20),
        name="pack_rows",
    )(targets, loss_mask, parts, residual)


def norm_kernel(blocks_ref, post_ref, final_ref, head_ref, tail_ref, turn_ref):
    n_z = blocks_ref.shape[0]
    per, cut = head_ref.shape
    dim = post_ref.shape[1]
    cols = dim // n_z
    rest, width = turn_ref.shape[1] // n_z, blocks_ref.shape[2]
    f32 = jnp.float32
    pieces = []
    for i in range(n_z):
        high = blocks_ref[i, :per, :cols].astype(f32)
        low = blocks_ref[i, :per, cols:].astype(f32)
        pieces += [high[:, : width - cols] + low, high[:, width - cols :]]
    ffn = jnp.concatenate(pieces, axis=1)
    for i in range(n_z):
        for c in range(width // LANES):
            turn_ref[c, i * rest : (i + 1) * rest] = blocks_ref[
                i, per:, c * LANES : (c + 1) * LANES
            ].astype(f32)

    def turned(r, c):
        return turn_ref[c, pl.ds(r, n_z, stride=rest), :]

    res = jnp.concatenate(
        [turned(r, c) for r in range(dim // width) for c in range(width // LANES)], axis=1
    )
    scale = lax.rsqrt(jnp.sum(ffn * ffn, axis=1, keepdims=True) / dim + EPS)
    stream = res + ffn * scale * post_ref[...]
    scale = lax.rsqrt(jnp.sum(stream * stream, axis=1, keepdims=True) / dim + EPS)
    states = (stream * scale * final_ref[...]).astype(jnp.bfloat16)
    head_ref[...] = states[:, :cut]
    tail = jnp.concatenate([states[:, cut:], turned(dim // width, 0).astype(jnp.bfloat16)], axis=1)
    tail_ref[...] = jnp.broadcast_to(tail[None], tail_ref.shape)


def norm_rows(blocks, post_gain, final_gain, per, cut, copies):
    n_z, rows, width = blocks.shape
    dim = post_gain.shape[0]
    return pl.pallas_call(
        norm_kernel,
        in_specs=[VMEM] * 3,
        out_shape=(
            jax.ShapeDtypeStruct((per, cut), blocks.dtype),
            jax.ShapeDtypeStruct((copies, per, dim - cut + LANES), blocks.dtype),
        ),
        scratch_shapes=[pltpu.VMEM((width // LANES, n_z * (rows - per), LANES), jnp.float32)],
        compiler_params=pltpu.CompilerParams(vmem_limit_bytes=8 << 20),
        name="norm_rows",
    )(blocks, post_gain[None], final_gain[None])


def sums_kernel(n_z, halves, embed_ref, out_ref, mask_ref, st_ref, acc_ref):
    n_s, held, _ = st_ref.shape
    dim, vocab = embed_ref.shape
    z, x, s = (lax.axis_index(a) for a in ("fsdp", "mp", "sub"))
    first = ((z * lax.axis_size("mp") + x) * n_s + s) * vocab
    for h in range(n_s):
        st_ref[h] = halves[h][...]
    states = st_ref.reshape(n_s * held, st_ref.shape[2])
    acc_ref[...] = dot_f32(states[:, :dim], embed_ref[...], ((1,), (0,)))
    digits = states[:, dim:].astype(jnp.float32)
    goal = digits[:, 0:1] + 256.0 * digits[:, 1:2] + 65536.0 * digits[:, 2:3]
    goal = goal.astype(jnp.int32) - first
    sums = jnp.zeros((n_s * held, LANES), jnp.float32)
    hits = jnp.zeros((n_s * held, LANES), jnp.float32)
    for v in range(0, vocab, LANES):
        capped = CAP * jnp.tanh(acc_ref[:, v : v + LANES] / CAP)
        ids = lax.broadcasted_iota(jnp.int32, capped.shape, 1) + v
        sums += jnp.exp(capped)
        hits += jnp.where(ids == goal, capped, 0.0)
    rows = [jnp.sum(r.T, axis=0, keepdims=True) for r in (sums, hits)]
    rows.append(digits.T[3:4])
    place = lax.broadcasted_iota(jnp.int32, (1, held), 1)
    core = (place + place // n_z + z + x + s) % n_s
    parts = [
        jnp.where(core == h, row[:, :held], row[:, held:]) for row in rows for h in range(n_s)
    ]
    mask_ref[...] = jnp.concatenate(parts[2 * n_s :], axis=0)
    part = jnp.concatenate(parts[: 2 * n_s], axis=0)
    out_ref[...] = jnp.broadcast_to(part[None], out_ref.shape)


def vocab_sums(halves, embed, n_z, copies):
    n_s, (held, width) = len(halves), halves[0].shape
    dim, vocab = embed.shape

    def kernel(*refs):
        sums_kernel(n_z, refs[:n_s], *refs[n_s:])

    return pl.pallas_call(
        kernel,
        in_specs=[VMEM] * (n_s + 1),
        out_shape=(
            jax.ShapeDtypeStruct((copies, 2 * n_s, held), jnp.float32),
            jax.ShapeDtypeStruct((n_s, held), jnp.float32),
        ),
        scratch_shapes=[
            pltpu.VMEM((n_s, held, width), jnp.bfloat16),
            pltpu.VMEM((n_s * held, vocab), jnp.float32),
        ],
        compiler_params=pltpu.CompilerParams(vmem_limit_bytes=24 << 20),
        cost_estimate=pl.CostEstimate(
            flops=2 * n_s * held * vocab * dim,
            bytes_accessed=2 * (n_s * held + vocab) * dim,
            transcendentals=2 * n_s * held * vocab,
        ),
        name="vocab_sums",
    )(*halves, embed)


def loss_kernel(n_z, packed_ref, mask_ref, token_ref, mean_ref):
    toks = token_ref.shape[0]
    n_s, held = mask_ref.shape
    z, s = lax.axis_index("fsdp"), lax.axis_index("sub")
    packed = jnp.sum(packed_ref[...], axis=0)
    sums, goals, mask = packed[:n_s], packed[n_s:], mask_ref[...]
    losses = mask * (jnp.log(sums) - goals)
    total, count = jnp.sum(losses), jnp.sum(mask)
    whole = jnp.full((1, held), total) / jnp.maximum(jnp.full((1, held), count), 1.0)
    mean_ref[...] = whole[0, :1]
    core = lax.broadcasted_iota(jnp.int32, losses.shape, 0)
    mine = jnp.sum(jnp.where(core == s, losses, 0.0), axis=0, keepdims=True)
    row = lax.broadcasted_iota(jnp.int32, (held, held), 0)
    lane = lax.broadcasted_iota(jnp.int32, (held, held), 1)
    spread = jnp.where((lane == row * n_z + z) & (row < toks), mine, 0.0)
    token_ref[...] = jnp.sum(spread.T, axis=0)[:toks]


def losses_of(packed, mask, n_z, toks):
    return pl.pallas_call(
        functools.partial(loss_kernel, n_z),
        in_specs=[VMEM, VMEM],
        out_shape=(
            jax.ShapeDtypeStruct((toks,), jnp.float32),
            jax.ShapeDtypeStruct((1,), jnp.float32),
        ),
        compiler_params=pltpu.CompilerParams(vmem_limit_bytes=4 << 20),
        name="losses_of",
    )(packed, mask)


def on_device(
    hidden,
    residual,
    down_packed,
    down_scale,
    post_gain,
    final_gain,
    embed_packed,
    embed_scale,
    targets,
    loss_mask,
):
    toks, width = hidden.shape
    n_z, n_x, n_s = (lax.axis_size(a) for a in ("fsdp", "mp", "sub"))
    cols = down_packed.shape[1]
    dim = n_z * cols
    held = n_z * toks
    per_x = held // n_x

    cut = gather_cut(toks, width, n_z)
    head, tail = split_columns(hidden, cut, n_z)
    tail = exchange_ring(tail, "fsdp")
    head = gather_ring(head, "fsdp")
    weight = dequant_down(down_packed, down_scale)
    part = dot_f32(head.reshape(held, cut), weight[:cut], ((1,), (0,))) + dot_f32(
        tail.reshape(held, width - cut), weight[cut:], ((1,), (0,))
    )

    part = jnp.swapaxes(part.reshape(n_z, toks, cols), 0, 1).reshape(n_x, per_x, cols)
    parts = lax.all_to_all(part, "mp", 0, 0, tiled=True)
    parts, residual, targets = lax.optimization_barrier((parts, residual, targets))

    block = pack_rows(targets, loss_mask, parts, residual)
    blocks = gather_ring(block, "fsdp")
    blocks, post_gain, final_gain = lax.optimization_barrier((blocks, post_gain, final_gain))

    cut = gather_cut(per_x, dim, n_x)
    head, tail = norm_rows(blocks, post_gain, final_gain, per_x, cut, n_x)
    tail = exchange_ring(tail, "mp")
    head = gather_ring(head, "mp")
    own = jnp.concatenate([head.reshape(held, cut), tail.reshape(held, dim - cut + LANES)], axis=1)
    far = lax.ppermute(own, "sub", [(i, n_s - 1 - i) for i in range(n_s)])
    embed = dequant_embed(embed_packed, embed_scale)
    packed, mask = vocab_sums((own, far), embed.T, n_z, n_x * n_s)

    packed = jnp.sum(lax.all_to_all(packed, ("mp", "sub"), 0, 0, tiled=True), axis=0)
    return losses_of(copy_for_each(packed, "fsdp"), mask, n_z, toks)


def solution(mesh):
    return jax.shard_map(
        on_device,
        mesh=mesh,
        in_specs=(
            P(("groups", "fsdp", "sub"), "mp"),
            P(("groups", "fsdp", "sub"), None),
            P("mp", "fsdp"),
            P("mp", "fsdp"),
            P(),
            P(),
            P(("fsdp", "mp", "sub"), None),
            P(("fsdp", "mp", "sub"), None),
            P(("groups", "fsdp", "sub")),
            P(("groups", "fsdp", "sub")),
        ),
        out_specs=(P(("groups", "fsdp", "sub")), P("groups")),
        check_vma=False,
    )
```

```python
import functools

import jax
import jax.numpy as jnp
from jax import lax
from jax.experimental import pallas as pl
from jax.experimental.pallas import tpu as pltpu
from jax.sharding import PartitionSpec as P


EPS = 1e-06
CAP = 30.0
GATHER_BYTES = 1 << 20
LANES = 128
DIGITS = 4
VMEM = pl.BlockSpec(memory_space=pltpu.VMEM)
SMEM = pl.BlockSpec(memory_space=pltpu.SMEM)


def copy_for_each(value, axis):
    peers = lax.axis_size(axis)
    return lax.all_to_all(
        jnp.broadcast_to(value[None], (peers, *value.shape)), axis, 0, 0, tiled=True
    )


def rings(axis):
    n, n_s = lax.axis_size(axis), lax.axis_size("sub")
    return [[i * n_s + (i + r) % n_s for i in range(n)] for r in range(n_s)]


def gather_ring(value, axis):
    return lax.all_gather(value, (axis, "sub"), axis_index_groups=rings(axis))


def exchange_ring(copies, axis):
    return lax.all_to_all(
        copies, (axis, "sub"), 0, 0, tiled=True, axis_index_groups=rings(axis)
    )


def gather_cut(rows, cols, peers):
    fit = (GATHER_BYTES - 1) // (peers * rows * 2)
    return min(cols, fit // LANES * LANES)


def signed_planes(words):
    shifts = (28 - 4 * jnp.arange(8, dtype=jnp.int32))[None, :, None]
    lifted = jnp.left_shift(words[:, None, :], shifts)
    return jnp.right_shift(lifted, 28)


def dequant_down(words, scales):
    cols = words.shape[1]
    codes = signed_planes(words).astype(jnp.bfloat16)
    grouped = codes.reshape(scales.shape[0], -1, cols) * scales[:, None, :]
    return grouped.reshape(-1, cols)


def dequant_embed(words, scales):
    rows = words.shape[0]
    codes = signed_planes(words).astype(jnp.bfloat16)
    grouped = codes.reshape(rows, scales.shape[1], -1) * scales[:, :, None]
    return grouped.reshape(rows, -1)


def dot_f32(a, b, dims):
    return lax.dot_general(a, b, (dims, ((), ())), preferred_element_type=jnp.float32)


def split_kernel(hidden_ref, head_ref, tail_ref):
    cut = head_ref.shape[1]
    head_ref[...] = hidden_ref[:, :cut]
    tail_ref[...] = jnp.broadcast_to(hidden_ref[:, cut:][None], tail_ref.shape)


def split_columns(hidden, cut, copies):
    rows, width = hidden.shape
    return pl.pallas_call(
        split_kernel,
        in_specs=[VMEM],
        out_shape=(
            jax.ShapeDtypeStruct((rows, cut), hidden.dtype),
            jax.ShapeDtypeStruct((copies, rows, width - cut), hidden.dtype),
        ),
        compiler_params=pltpu.CompilerParams(vmem_limit_bytes=4 << 20),
        name="split_columns",
    )(hidden)


def pack_kernel(targets_ref, loss_mask_ref, parts_ref, residual_ref, out_ref):
    per, cols = parts_ref.shape[1:]
    width = out_ref.shape[1]
    ffn = jnp.sum(parts_ref[...], axis=0)
    high = ffn.astype(jnp.bfloat16)
    low = (ffn - high.astype(jnp.float32)).astype(jnp.bfloat16)
    out_ref[:per, :cols] = high
    out_ref[:per, cols:] = low[:, : width - cols]
    x = lax.axis_index("mp")
    res = residual_ref[...].astype(jnp.float32)
    token = lax.broadcasted_iota(jnp.int32, res.shape, 0)
    res = jnp.sum(jnp.where(token == x, res, 0.0), axis=0, keepdims=True)
    rows = [res[:, c : c + width] for c in range(0, res.shape[1], width)]
    lane = lax.broadcasted_iota(jnp.int32, (1, width), 1)
    digit = jnp.zeros((1, width), jnp.int32)
    for i in range(targets_ref.shape[0]):
        goal = targets_ref[i]
        values = (goal & 255, (goal >> 8) & 255, goal >> 16, loss_mask_ref[i])
        for v, value in enumerate(values):
            digit = jnp.where(lane == DIGITS * i + v, value, digit)
    rows.append(digit.astype(jnp.float32))
    rows.append(jnp.zeros((out_ref.shape[0] - per - len(rows), width), jnp.float32))
    out_ref[per:] = jnp.concatenate(rows, axis=0).astype(jnp.bfloat16)


def pack_rows(targets, loss_mask, parts, residual):
    per, cols = parts.shape[1:]
    width = cols + -cols % LANES
    count = per + residual.shape[1] // width + 1
    return pl.pallas_call(
        pack_kernel,
        in_specs=[SMEM, SMEM, VMEM, VMEM],
        out_shape=jax.ShapeDtypeStruct((count + -count % 16, width), jnp.bfloat16),
        compiler_params=pltpu.CompilerParams(vmem_limit_bytes=4 << 20),
        name="pack_rows",
    )(targets, loss_mask, parts, residual)


def norm_kernel(blocks_ref, post_ref, final_ref, head_ref, tail_ref, digit_ref, turn_ref):
    n_z = blocks_ref.shape[0]
    per, cut = head_ref.shape
    dim = post_ref.shape[1]
    cols = dim // n_z
    rest, width = turn_ref.shape[1] // n_z, blocks_ref.shape[2]
    f32 = jnp.float32
    pieces = []
    for i in range(n_z):
        high = blocks_ref[i, :per, :cols].astype(f32)
        low = blocks_ref[i, :per, cols:].astype(f32)
        pieces += [high[:, : width - cols] + low, high[:, width - cols :]]
    ffn = jnp.concatenate(pieces, axis=1)
    for i in range(n_z):
        for c in range(width // LANES):
            turn_ref[c, i * rest : (i + 1) * rest] = blocks_ref[
                i, per:, c * LANES : (c + 1) * LANES
            ].astype(f32)

    def turned(r, c):
        return turn_ref[c, pl.ds(r, n_z, stride=rest), :]

    res = jnp.concatenate(
        [turned(r, c) for r in range(dim // width) for c in range(width // LANES)], axis=1
    )
    scale = lax.rsqrt(jnp.sum(ffn * ffn, axis=1, keepdims=True) / dim + EPS)
    stream = res + ffn * scale * post_ref[...]
    scale = lax.rsqrt(jnp.sum(stream * stream, axis=1, keepdims=True) / dim + EPS)
    states = (stream * scale * final_ref[...]).astype(jnp.bfloat16)
    head_ref[...] = states[:, :cut]
    tail_ref[...] = jnp.broadcast_to(states[:, cut:][None], tail_ref.shape)
    digits = turned(dim // width, 0)
    rows = [digits] + [
        pltpu.roll(digits, LANES - DIGITS * i, axis=1) for i in range(1, digit_ref.shape[0] // n_z)
    ]
    digit_ref[...] = jnp.concatenate(rows, axis=0).astype(jnp.bfloat16)


def norm_rows(blocks, post_gain, final_gain, per, cut, copies, toks):
    n_z, rows, width = blocks.shape
    dim = post_gain.shape[0]
    return pl.pallas_call(
        norm_kernel,
        in_specs=[VMEM] * 3,
        out_shape=(
            jax.ShapeDtypeStruct((per, cut), blocks.dtype),
            jax.ShapeDtypeStruct((copies, per, dim - cut), blocks.dtype),
            jax.ShapeDtypeStruct((toks * n_z, LANES), blocks.dtype),
        ),
        scratch_shapes=[pltpu.VMEM((width // LANES, n_z * (rows - per), LANES), jnp.float32)],
        compiler_params=pltpu.CompilerParams(vmem_limit_bytes=8 << 20),
        name="norm_rows",
    )(blocks, post_gain[None], final_gain[None])


def sums_kernel(n_z, halves, embed_ref, out_ref, mask_ref, st_ref, acc_ref):
    n_s, held, _ = st_ref.shape
    dim, vocab = embed_ref.shape
    z, x, s = (lax.axis_index(a) for a in ("fsdp", "mp", "sub"))
    first = ((z * lax.axis_size("mp") + x) * n_s + s) * vocab
    for h in range(n_s):
        st_ref[h] = halves[h][...]
    states = st_ref.reshape(n_s * held, st_ref.shape[2])
    acc_ref[...] = dot_f32(states[:, :dim], embed_ref[...], ((1,), (0,)))
    rings_of = [half[:, dim:].astype(jnp.float32) for half in halves]
    token = lax.broadcasted_iota(jnp.int32, rings_of[0].shape, 0) // n_z
    digits = jnp.concatenate(
        [
            jnp.where((token + x) % n_s == 0, rings_of[h], rings_of[n_s - 1 - h])
            for h in range(n_s)
        ],
        axis=0,
    )
    goal = digits[:, 0:1] + 256.0 * digits[:, 1:2] + 65536.0 * digits[:, 2:3]
    goal = goal.astype(jnp.int32) - first
    sums = jnp.zeros((n_s * held, LANES), jnp.float32)
    hits = jnp.zeros((n_s * held, LANES), jnp.float32)
    for v in range(0, vocab, LANES):
        capped = CAP * jnp.tanh(acc_ref[:, v : v + LANES] / CAP)
        ids = lax.broadcasted_iota(jnp.int32, capped.shape, 1) + v
        sums += jnp.exp(capped)
        hits += jnp.where(ids == goal, capped, 0.0)
    rows = [jnp.sum(r.T, axis=0, keepdims=True) for r in (sums, hits)]
    rows.append(digits.T[3:4])
    place = lax.broadcasted_iota(jnp.int32, (1, held), 1)
    core = (place + place // n_z + z + x + s) % n_s
    parts = [
        jnp.where(core == h, row[:, :held], row[:, held:]) for row in rows for h in range(n_s)
    ]
    mask_ref[...] = jnp.concatenate(parts[2 * n_s :], axis=0)
    part = jnp.concatenate(parts[: 2 * n_s], axis=0)
    out_ref[...] = jnp.broadcast_to(part[None], out_ref.shape)


def vocab_sums(halves, embed, n_z, copies):
    n_s, (held, width) = len(halves), halves[0].shape
    dim, vocab = embed.shape

    def kernel(*refs):
        sums_kernel(n_z, refs[:n_s], *refs[n_s:])

    return pl.pallas_call(
        kernel,
        in_specs=[VMEM] * (n_s + 1),
        out_shape=(
            jax.ShapeDtypeStruct((copies, 2 * n_s, held), jnp.float32),
            jax.ShapeDtypeStruct((n_s, held), jnp.float32),
        ),
        scratch_shapes=[
            pltpu.VMEM((n_s, held, width), jnp.bfloat16),
            pltpu.VMEM((n_s * held, vocab), jnp.float32),
        ],
        compiler_params=pltpu.CompilerParams(vmem_limit_bytes=24 << 20),
        cost_estimate=pl.CostEstimate(
            flops=2 * n_s * held * vocab * dim,
            bytes_accessed=2 * (n_s * held + vocab) * dim,
            transcendentals=2 * n_s * held * vocab,
        ),
        name="vocab_sums",
    )(*halves, embed)


def loss_kernel(n_z, packed_ref, mask_ref, token_ref, mean_ref):
    toks = token_ref.shape[0]
    n_s, held = mask_ref.shape
    z, s = lax.axis_index("fsdp"), lax.axis_index("sub")
    packed = jnp.sum(packed_ref[...], axis=0)
    sums, goals, mask = packed[:n_s], packed[n_s:], mask_ref[...]
    losses = mask * (jnp.log(sums) - goals)
    total, count = jnp.sum(losses), jnp.sum(mask)
    whole = jnp.full((1, held), total) / jnp.maximum(jnp.full((1, held), count), 1.0)
    mean_ref[...] = whole[0, :1]
    core = lax.broadcasted_iota(jnp.int32, losses.shape, 0)
    mine = jnp.sum(jnp.where(core == s, losses, 0.0), axis=0, keepdims=True)
    row = lax.broadcasted_iota(jnp.int32, (held, held), 0)
    lane = lax.broadcasted_iota(jnp.int32, (held, held), 1)
    spread = jnp.where((lane == row * n_z + z) & (row < toks), mine, 0.0)
    token_ref[...] = jnp.sum(spread.T, axis=0)[:toks]


def losses_of(packed, mask, n_z, toks):
    return pl.pallas_call(
        functools.partial(loss_kernel, n_z),
        in_specs=[VMEM, VMEM],
        out_shape=(
            jax.ShapeDtypeStruct((toks,), jnp.float32),
            jax.ShapeDtypeStruct((1,), jnp.float32),
        ),
        compiler_params=pltpu.CompilerParams(vmem_limit_bytes=4 << 20),
        name="losses_of",
    )(packed, mask)


def on_device(
    hidden,
    residual,
    down_packed,
    down_scale,
    post_gain,
    final_gain,
    embed_packed,
    embed_scale,
    targets,
    loss_mask,
):
    toks, width = hidden.shape
    n_z, n_x, n_s = (lax.axis_size(a) for a in ("fsdp", "mp", "sub"))
    cols = down_packed.shape[1]
    dim = n_z * cols
    held = n_z * toks
    per_x = held // n_x

    cut = gather_cut(toks, width, n_z)
    head, tail = split_columns(hidden, cut, n_z)
    tail = exchange_ring(tail, "fsdp")
    head = gather_ring(head, "fsdp")
    weight = dequant_down(down_packed, down_scale)
    part = dot_f32(head.reshape(held, cut), weight[:cut], ((1,), (0,))) + dot_f32(
        tail.reshape(held, width - cut), weight[cut:], ((1,), (0,))
    )

    part = jnp.swapaxes(part.reshape(n_z, toks, cols), 0, 1).reshape(n_x, per_x, cols)
    parts = lax.all_to_all(part, "mp", 0, 0, tiled=True)
    parts, residual, targets = lax.optimization_barrier((parts, residual, targets))

    block = pack_rows(targets, loss_mask, parts, residual)
    blocks = gather_ring(block, "fsdp")
    blocks, post_gain, final_gain = lax.optimization_barrier((blocks, post_gain, final_gain))

    cut = gather_cut(per_x, dim, n_x)
    head, tail, digits = norm_rows(blocks, post_gain, final_gain, per_x, cut, n_x, toks)
    tail = exchange_ring(tail, "mp")
    head = gather_ring(head, "mp")
    own = [head.reshape(held, cut), tail.reshape(held, dim - cut), digits]
    own = jnp.concatenate(own, axis=1)
    far = lax.ppermute(own, "sub", [(i, n_s - 1 - i) for i in range(n_s)])
    embed = dequant_embed(embed_packed, embed_scale)
    packed, mask = vocab_sums((own, far), embed.T, n_z, n_x * n_s)

    packed = jnp.sum(lax.all_to_all(packed, ("mp", "sub"), 0, 0, tiled=True), axis=0)
    return losses_of(copy_for_each(packed, "fsdp"), mask, n_z, toks)


def solution(mesh):
    return jax.shard_map(
        on_device,
        mesh=mesh,
        in_specs=(
            P(("groups", "fsdp", "sub"), "mp"),
            P(("groups", "fsdp", "sub"), None),
            P("mp", "fsdp"),
            P("mp", "fsdp"),
            P(),
            P(),
            P(("fsdp", "mp", "sub"), None),
            P(("fsdp", "mp", "sub"), None),
            P(("groups", "fsdp", "sub")),
            P(("groups", "fsdp", "sub")),
        ),
        out_specs=(P(("groups", "fsdp", "sub")), P("groups")),
        check_vma=False,
    )
```

```python
import functools

import jax
import jax.numpy as jnp
from jax import lax
from jax.experimental import pallas as pl
from jax.experimental.pallas import tpu as pltpu
from jax.sharding import PartitionSpec as P


EPS = 1e-06
CAP = 30.0
GATHER_BYTES = 1 << 20
LANES = 128
DIGITS = 4
VMEM = pl.BlockSpec(memory_space=pltpu.VMEM)
SMEM = pl.BlockSpec(memory_space=pltpu.SMEM)


def copy_for_each(value, axis):
    peers = lax.axis_size(axis)
    return lax.all_to_all(
        jnp.broadcast_to(value[None], (peers, *value.shape)), axis, 0, 0, tiled=True
    )


def rings(axis):
    n, n_s = lax.axis_size(axis), lax.axis_size("sub")
    return [[i * n_s + (i + r) % n_s for i in range(n)] for r in range(n_s)]


def gather_ring(value, axis):
    return lax.all_gather(value, (axis, "sub"), axis_index_groups=rings(axis))


def exchange_ring(copies, axis):
    return lax.all_to_all(
        copies, (axis, "sub"), 0, 0, tiled=True, axis_index_groups=rings(axis)
    )


def gather_cut(rows, cols, peers):
    fit = (GATHER_BYTES - 1) // (peers * rows * 2)
    return min(cols, fit // LANES * LANES)


def signed_planes(words):
    shifts = (28 - 4 * jnp.arange(8, dtype=jnp.int32))[None, :, None]
    lifted = jnp.left_shift(words[:, None, :], shifts)
    return jnp.right_shift(lifted, 28)


def dequant_down(words, scales):
    cols = words.shape[1]
    codes = signed_planes(words).astype(jnp.bfloat16)
    grouped = codes.reshape(scales.shape[0], -1, cols) * scales[:, None, :]
    return grouped.reshape(-1, cols)


def dequant_embed(words, scales):
    rows = words.shape[0]
    codes = signed_planes(words).astype(jnp.bfloat16)
    grouped = codes.reshape(rows, scales.shape[1], -1) * scales[:, :, None]
    return grouped.reshape(rows, -1)


def dot_f32(a, b, dims):
    return lax.dot_general(a, b, (dims, ((), ())), preferred_element_type=jnp.float32)


def split_kernel(hidden_ref, head_ref, tail_ref):
    cut = head_ref.shape[1]
    head_ref[...] = hidden_ref[:, :cut]
    tail_ref[...] = jnp.broadcast_to(hidden_ref[:, cut:][None], tail_ref.shape)


def split_columns(hidden, cut, copies):
    rows, width = hidden.shape
    return pl.pallas_call(
        split_kernel,
        in_specs=[VMEM],
        out_shape=(
            jax.ShapeDtypeStruct((rows, cut), hidden.dtype),
            jax.ShapeDtypeStruct((copies, rows, width - cut), hidden.dtype),
        ),
        compiler_params=pltpu.CompilerParams(vmem_limit_bytes=4 << 20),
        name="split_columns",
    )(hidden)


def pack_kernel(targets_ref, loss_mask_ref, parts_ref, residual_ref, out_ref):
    per, cols = parts_ref.shape[1:]
    width = out_ref.shape[1]
    ffn = jnp.sum(parts_ref[...], axis=0)
    high = ffn.astype(jnp.bfloat16)
    low = ffn - high.astype(jnp.float32)
    spare, half = width - cols, per // 2
    out_ref[:per, :cols] = high
    out_ref[:per, cols:] = low[:, :spare].astype(jnp.bfloat16)
    low = jnp.concatenate([low[:half, spare:], low[half:, spare:]], axis=1)
    out_ref[per : per + half] = low.astype(jnp.bfloat16)
    x = lax.axis_index("mp")
    res = residual_ref[...].astype(jnp.float32)
    token = lax.broadcasted_iota(jnp.int32, res.shape, 0)
    res = jnp.sum(jnp.where(token == x, res, 0.0), axis=0, keepdims=True)
    rows = [res[:, c : c + width] for c in range(0, res.shape[1], width)]
    lane = lax.broadcasted_iota(jnp.int32, (1, width), 1)
    digit = jnp.zeros((1, width), jnp.int32)
    for i in range(targets_ref.shape[0]):
        goal = targets_ref[i]
        values = (goal & 255, (goal >> 8) & 255, goal >> 16, loss_mask_ref[i])
        for v, value in enumerate(values):
            digit = jnp.where(lane == DIGITS * i + v, value, digit)
    rows.append(digit.astype(jnp.float32))
    rows.append(jnp.zeros((out_ref.shape[0] - per - half - len(rows), width), jnp.float32))
    out_ref[per + half :] = jnp.concatenate(rows, axis=0).astype(jnp.bfloat16)


def pack_rows(targets, loss_mask, parts, residual):
    per, cols = parts.shape[1:]
    width = cols + -cols % LANES
    count = per + per // 2 + residual.shape[1] // width + 1
    return pl.pallas_call(
        pack_kernel,
        in_specs=[SMEM, SMEM, VMEM, VMEM],
        out_shape=jax.ShapeDtypeStruct((count + -count % 8, width), jnp.bfloat16),
        compiler_params=pltpu.CompilerParams(vmem_limit_bytes=4 << 20),
        name="pack_rows",
    )(targets, loss_mask, parts, residual)


def norm_kernel(blocks_ref, post_ref, final_ref, head_ref, tail_ref, digit_ref, turn_ref):
    n_z = blocks_ref.shape[0]
    per, cut = head_ref.shape
    dim = post_ref.shape[1]
    cols = dim // n_z
    rest, width = turn_ref.shape[1] // n_z, blocks_ref.shape[2]
    f32 = jnp.float32
    lead = per + per // 2
    pieces = []
    for i in range(n_z):
        high = blocks_ref[i, :per, :cols].astype(f32)
        low = blocks_ref[i, :per, cols:].astype(f32)
        rest_low = blocks_ref[i, per:lead].astype(f32)
        rest_low = jnp.concatenate([rest_low[:, : width // 2], rest_low[:, width // 2 :]], axis=0)
        pieces += [high[:, : width - cols] + low, high[:, width - cols :] + rest_low]
    ffn = jnp.concatenate(pieces, axis=1)
    for i in range(n_z):
        for c in range(width // LANES):
            turn_ref[c, i * rest : (i + 1) * rest] = blocks_ref[
                i, lead:, c * LANES : (c + 1) * LANES
            ].astype(f32)

    def turned(r, c):
        return turn_ref[c, pl.ds(r, n_z, stride=rest), :]

    res = jnp.concatenate(
        [turned(r, c) for r in range(dim // width) for c in range(width // LANES)], axis=1
    )
    scale = lax.rsqrt(jnp.sum(ffn * ffn, axis=1, keepdims=True) / dim + EPS)
    stream = res + ffn * scale * post_ref[...]
    scale = lax.rsqrt(jnp.sum(stream * stream, axis=1, keepdims=True) / dim + EPS)
    states = (stream * scale * final_ref[...]).astype(jnp.bfloat16)
    head_ref[...] = states[:, :cut]
    tail_ref[...] = jnp.broadcast_to(states[:, cut:][None], tail_ref.shape)
    digits = turned(dim // width, 0)
    rows = [digits] + [
        pltpu.roll(digits, LANES - DIGITS * i, axis=1) for i in range(1, digit_ref.shape[0] // n_z)
    ]
    digit_ref[...] = jnp.concatenate(rows, axis=0).astype(jnp.bfloat16)


def norm_rows(blocks, post_gain, final_gain, per, cut, copies, toks):
    n_z, rows, width = blocks.shape
    dim = post_gain.shape[0]
    return pl.pallas_call(
        norm_kernel,
        in_specs=[VMEM] * 3,
        out_shape=(
            jax.ShapeDtypeStruct((per, cut), blocks.dtype),
            jax.ShapeDtypeStruct((copies, per, dim - cut), blocks.dtype),
            jax.ShapeDtypeStruct((toks * n_z, LANES), blocks.dtype),
        ),
        scratch_shapes=[pltpu.VMEM((width // LANES, n_z * (rows - per - per // 2), LANES), jnp.float32)],
        compiler_params=pltpu.CompilerParams(vmem_limit_bytes=8 << 20),
        name="norm_rows",
    )(blocks, post_gain[None], final_gain[None])


def sums_kernel(n_z, halves, embed_ref, out_ref, mask_ref, st_ref, acc_ref):
    n_s, held, _ = st_ref.shape
    dim, vocab = embed_ref.shape
    z, x, s = (lax.axis_index(a) for a in ("fsdp", "mp", "sub"))
    first = ((z * lax.axis_size("mp") + x) * n_s + s) * vocab
    for h in range(n_s):
        st_ref[h] = halves[h][...]
    states = st_ref.reshape(n_s * held, st_ref.shape[2])
    acc_ref[...] = dot_f32(states[:, :dim], embed_ref[...], ((1,), (0,)))
    rings_of = [half[:, dim:].astype(jnp.float32) for half in halves]
    token = lax.broadcasted_iota(jnp.int32, rings_of[0].shape, 0) // n_z
    digits = jnp.concatenate(
        [
            jnp.where((token + x) % n_s == 0, rings_of[h], rings_of[n_s - 1 - h])
            for h in range(n_s)
        ],
        axis=0,
    )
    goal = digits[:, 0:1] + 256.0 * digits[:, 1:2] + 65536.0 * digits[:, 2:3]
    goal = goal.astype(jnp.int32) - first
    sums = jnp.zeros((n_s * held, LANES), jnp.float32)
    hits = jnp.zeros((n_s * held, LANES), jnp.float32)
    for v in range(0, vocab, LANES):
        capped = CAP * jnp.tanh(acc_ref[:, v : v + LANES] / CAP)
        ids = lax.broadcasted_iota(jnp.int32, capped.shape, 1) + v
        sums += jnp.exp(capped)
        hits += jnp.where(ids == goal, capped, 0.0)
    rows = [jnp.sum(r.T, axis=0, keepdims=True) for r in (sums, hits)]
    rows.append(digits.T[3:4])
    place = lax.broadcasted_iota(jnp.int32, (1, held), 1)
    core = (place + place // n_z + z + x + s) % n_s
    parts = [
        jnp.where(core == h, row[:, :held], row[:, held:]) for row in rows for h in range(n_s)
    ]
    mask_ref[...] = jnp.concatenate(parts[2 * n_s :], axis=0)
    part = jnp.concatenate(parts[: 2 * n_s], axis=0)
    out_ref[...] = jnp.broadcast_to(part[None], out_ref.shape)


def vocab_sums(halves, embed, n_z, copies):
    n_s, (held, width) = len(halves), halves[0].shape
    dim, vocab = embed.shape

    def kernel(*refs):
        sums_kernel(n_z, refs[:n_s], *refs[n_s:])

    return pl.pallas_call(
        kernel,
        in_specs=[VMEM] * (n_s + 1),
        out_shape=(
            jax.ShapeDtypeStruct((copies, 2 * n_s, held), jnp.float32),
            jax.ShapeDtypeStruct((n_s, held), jnp.float32),
        ),
        scratch_shapes=[
            pltpu.VMEM((n_s, held, width), jnp.bfloat16),
            pltpu.VMEM((n_s * held, vocab), jnp.float32),
        ],
        compiler_params=pltpu.CompilerParams(vmem_limit_bytes=24 << 20),
        cost_estimate=pl.CostEstimate(
            flops=2 * n_s * held * vocab * dim,
            bytes_accessed=2 * (n_s * held + vocab) * dim,
            transcendentals=2 * n_s * held * vocab,
        ),
        name="vocab_sums",
    )(*halves, embed)


def loss_kernel(n_z, packed_ref, mask_ref, token_ref, mean_ref):
    toks = token_ref.shape[0]
    n_s, held = mask_ref.shape
    z, s = lax.axis_index("fsdp"), lax.axis_index("sub")
    packed = jnp.sum(packed_ref[...], axis=0)
    sums, goals, mask = packed[:n_s], packed[n_s:], mask_ref[...]
    losses = mask * (jnp.log(sums) - goals)
    total, count = jnp.sum(losses), jnp.sum(mask)
    whole = jnp.full((1, held), total) / jnp.maximum(jnp.full((1, held), count), 1.0)
    mean_ref[...] = whole[0, :1]
    core = lax.broadcasted_iota(jnp.int32, losses.shape, 0)
    mine = jnp.sum(jnp.where(core == s, losses, 0.0), axis=0, keepdims=True)
    row = lax.broadcasted_iota(jnp.int32, (held, held), 0)
    lane = lax.broadcasted_iota(jnp.int32, (held, held), 1)
    spread = jnp.where((lane == row * n_z + z) & (row < toks), mine, 0.0)
    token_ref[...] = jnp.sum(spread.T, axis=0)[:toks]


def losses_of(packed, mask, n_z, toks):
    return pl.pallas_call(
        functools.partial(loss_kernel, n_z),
        in_specs=[VMEM, VMEM],
        out_shape=(
            jax.ShapeDtypeStruct((toks,), jnp.float32),
            jax.ShapeDtypeStruct((1,), jnp.float32),
        ),
        compiler_params=pltpu.CompilerParams(vmem_limit_bytes=4 << 20),
        name="losses_of",
    )(packed, mask)


def on_device(
    hidden,
    residual,
    down_packed,
    down_scale,
    post_gain,
    final_gain,
    embed_packed,
    embed_scale,
    targets,
    loss_mask,
):
    toks, width = hidden.shape
    n_z, n_x, n_s = (lax.axis_size(a) for a in ("fsdp", "mp", "sub"))
    cols = down_packed.shape[1]
    dim = n_z * cols
    held = n_z * toks
    per_x = held // n_x

    cut = gather_cut(toks, width, n_z)
    head, tail = split_columns(hidden, cut, n_z)
    tail = exchange_ring(tail, "fsdp")
    head = gather_ring(head, "fsdp")
    weight = dequant_down(down_packed, down_scale)
    part = dot_f32(head.reshape(held, cut), weight[:cut], ((1,), (0,))) + dot_f32(
        tail.reshape(held, width - cut), weight[cut:], ((1,), (0,))
    )

    part = jnp.swapaxes(part.reshape(n_z, toks, cols), 0, 1).reshape(n_x, per_x, cols)
    parts = lax.all_to_all(part, "mp", 0, 0, tiled=True)
    parts, residual, targets = lax.optimization_barrier((parts, residual, targets))

    block = pack_rows(targets, loss_mask, parts, residual)
    blocks = gather_ring(block, "fsdp")
    blocks, post_gain, final_gain = lax.optimization_barrier((blocks, post_gain, final_gain))

    cut = gather_cut(per_x, dim, n_x)
    head, tail, digits = norm_rows(blocks, post_gain, final_gain, per_x, cut, n_x, toks)
    tail = exchange_ring(tail, "mp")
    head = gather_ring(head, "mp")
    own = [head.reshape(held, cut), tail.reshape(held, dim - cut), digits]
    own = jnp.concatenate(own, axis=1)
    far = lax.ppermute(own, "sub", [(i, n_s - 1 - i) for i in range(n_s)])
    embed = dequant_embed(embed_packed, embed_scale)
    packed, mask = vocab_sums((own, far), embed.T, n_z, n_x * n_s)

    packed = jnp.sum(lax.all_to_all(packed, ("mp", "sub"), 0, 0, tiled=True), axis=0)
    return losses_of(copy_for_each(packed, "fsdp"), mask, n_z, toks)


def solution(mesh):
    return jax.shard_map(
        on_device,
        mesh=mesh,
        in_specs=(
            P(("groups", "fsdp", "sub"), "mp"),
            P(("groups", "fsdp", "sub"), None),
            P("mp", "fsdp"),
            P("mp", "fsdp"),
            P(),
            P(),
            P(("fsdp", "mp", "sub"), None),
            P(("fsdp", "mp", "sub"), None),
            P(("groups", "fsdp", "sub")),
            P(("groups", "fsdp", "sub")),
        ),
        out_specs=(P(("groups", "fsdp", "sub")), P("groups")),
        check_vma=False,
    )
```

```python
import functools

import jax
import jax.numpy as jnp
from jax import lax
from jax.experimental import pallas as pl
from jax.experimental.pallas import tpu as pltpu
from jax.sharding import PartitionSpec as P


EPS = 1e-06
CAP = 30.0
GATHER_BYTES = 1 << 20
LANES = 128
DIGITS = 4
VMEM = pl.BlockSpec(memory_space=pltpu.VMEM)
SMEM = pl.BlockSpec(memory_space=pltpu.SMEM)


def copy_for_each(value, axis):
    peers = lax.axis_size(axis)
    return lax.all_to_all(
        jnp.broadcast_to(value[None], (peers, *value.shape)), axis, 0, 0, tiled=True
    )


def rings(axis):
    n, n_s = lax.axis_size(axis), lax.axis_size("sub")
    return [[i * n_s + (i + r) % n_s for i in range(n)] for r in range(n_s)]


def gather_ring(value, axis):
    return lax.all_gather(value, (axis, "sub"), axis_index_groups=rings(axis))


def exchange_ring(copies, axis):
    return lax.all_to_all(
        copies, (axis, "sub"), 0, 0, tiled=True, axis_index_groups=rings(axis)
    )


def gather_cut(rows, cols, peers):
    fit = (GATHER_BYTES - 1) // (peers * rows * 2)
    return min(cols, fit // LANES * LANES)


def signed_planes(words):
    shifts = (28 - 4 * jnp.arange(8, dtype=jnp.int32))[None, :, None]
    lifted = jnp.left_shift(words[:, None, :], shifts)
    return jnp.right_shift(lifted, 28)


def dequant_embed(words, scales):
    rows = words.shape[0]
    codes = signed_planes(words).astype(jnp.bfloat16)
    grouped = codes.reshape(rows, scales.shape[1], -1) * scales[:, :, None]
    return grouped.reshape(rows, -1)


def dot_f32(a, b, dims):
    return lax.dot_general(a, b, (dims, ((), ())), preferred_element_type=jnp.float32)


def split_kernel(span, hidden_ref, head_ref, tail_ref):
    rows, width = hidden_ref.shape
    cut = head_ref.shape[1]
    place = lax.broadcasted_iota(jnp.int32, (span, span), 1)
    unit = place % (span // 8) * 8 + place // (span // 8)
    order = jnp.where(lax.broadcasted_iota(jnp.int32, (span, span), 0) == unit, 1.0, 0.0)
    hidden = hidden_ref[...].astype(jnp.float32)
    tiles = [hidden[:, c : c + span] for c in range(0, width, span)]
    tiles = jnp.concatenate(tiles, axis=0).astype(jnp.bfloat16)
    turned = dot_f32(tiles, order.astype(jnp.bfloat16), ((1,), (0,)))
    for i, c in enumerate(range(0, width, span)):
        tile = turned[i * rows : (i + 1) * rows].astype(jnp.bfloat16)
        if c < cut:
            head_ref[:, c : c + span] = tile
        else:
            c -= cut
            tail_ref[:, :, c : c + span] = jnp.broadcast_to(
                tile[None], (tail_ref.shape[0], rows, span)
            )


def split_columns(hidden, cut, copies, span):
    rows, width = hidden.shape
    return pl.pallas_call(
        functools.partial(split_kernel, span),
        in_specs=[VMEM],
        out_shape=(
            jax.ShapeDtypeStruct((rows, cut), hidden.dtype),
            jax.ShapeDtypeStruct((copies, rows, width - cut), hidden.dtype),
        ),
        compiler_params=pltpu.CompilerParams(vmem_limit_bytes=4 << 20),
        name="split_columns",
    )(hidden)


def weight_kernel(words_ref, scale_ref, head_ref, tail_ref):
    cut = head_ref.shape[0]
    words = words_ref[...].T
    scale = scale_ref[...].astype(jnp.float32)
    groups = scale.shape[0]
    per = words.shape[0] // groups
    for g in range(groups):
        block = words[g * per : (g + 1) * per]
        for k in range(8):
            code = ((block << (28 - 4 * k)) >> 28).astype(jnp.float32)
            value = (code * scale[g : g + 1]).astype(jnp.bfloat16)
            row = (g * 8 + k) * per
            if row < cut:
                head_ref[row : row + per] = value
            else:
                tail_ref[row - cut : row - cut + per] = value


def down_weight(words, scale, cut):
    cols, rows = words.shape
    return pl.pallas_call(
        weight_kernel,
        in_specs=[VMEM] * 2,
        out_shape=(
            jax.ShapeDtypeStruct((cut, cols), scale.dtype),
            jax.ShapeDtypeStruct((8 * rows - cut, cols), scale.dtype),
        ),
        compiler_params=pltpu.CompilerParams(vmem_limit_bytes=12 << 20),
        name="down_weight",
    )(words, scale)


def pack_kernel(targets_ref, loss_mask_ref, parts_ref, residual_ref, out_ref):
    per, cols = parts_ref.shape[1:]
    width = out_ref.shape[1]
    ffn = jnp.sum(parts_ref[...], axis=0)
    high = ffn.astype(jnp.bfloat16)
    low = ffn - high.astype(jnp.float32)
    spare, half = width - cols, per // 2
    out_ref[:per, :cols] = high
    out_ref[:per, cols:] = low[:, :spare].astype(jnp.bfloat16)
    low = jnp.concatenate([low[:half, spare:], low[half:, spare:]], axis=1)
    out_ref[per : per + half] = low.astype(jnp.bfloat16)
    x = lax.axis_index("mp")
    res = residual_ref[...].astype(jnp.float32)
    token = lax.broadcasted_iota(jnp.int32, res.shape, 0)
    res = jnp.sum(jnp.where(token == x, res, 0.0), axis=0, keepdims=True)
    rows = [res[:, c : c + width] for c in range(0, res.shape[1], width)]
    lane = lax.broadcasted_iota(jnp.int32, (1, width), 1)
    digit = jnp.zeros((1, width), jnp.int32)
    for i in range(targets_ref.shape[0]):
        goal = targets_ref[i]
        values = (goal & 255, (goal >> 8) & 255, goal >> 16, loss_mask_ref[i])
        for v, value in enumerate(values):
            digit = jnp.where(lane == DIGITS * i + v, value, digit)
    rows.append(digit.astype(jnp.float32))
    rows.append(jnp.zeros((out_ref.shape[0] - per - half - len(rows), width), jnp.float32))
    out_ref[per + half :] = jnp.concatenate(rows, axis=0).astype(jnp.bfloat16)


def pack_rows(targets, loss_mask, parts, residual):
    per, cols = parts.shape[1:]
    width = cols + -cols % LANES
    count = per + per // 2 + residual.shape[1] // width + 1
    return pl.pallas_call(
        pack_kernel,
        in_specs=[SMEM, SMEM, VMEM, VMEM],
        out_shape=jax.ShapeDtypeStruct((count + -count % 8, width), jnp.bfloat16),
        compiler_params=pltpu.CompilerParams(vmem_limit_bytes=4 << 20),
        name="pack_rows",
    )(targets, loss_mask, parts, residual)


def norm_kernel(blocks_ref, post_ref, final_ref, head_ref, tail_ref, digit_ref, turn_ref):
    n_z = blocks_ref.shape[0]
    per, cut = head_ref.shape
    dim = post_ref.shape[1]
    cols = dim // n_z
    rest, width = turn_ref.shape[1] // n_z, blocks_ref.shape[2]
    f32 = jnp.float32
    lead = per + per // 2
    pieces = []
    for i in range(n_z):
        high = blocks_ref[i, :per, :cols].astype(f32)
        low = blocks_ref[i, :per, cols:].astype(f32)
        rest_low = blocks_ref[i, per:lead].astype(f32)
        rest_low = jnp.concatenate([rest_low[:, : width // 2], rest_low[:, width // 2 :]], axis=0)
        pieces += [high[:, : width - cols] + low, high[:, width - cols :] + rest_low]
    ffn = jnp.concatenate(pieces, axis=1)
    for i in range(n_z):
        for c in range(width // LANES):
            turn_ref[c, i * rest : (i + 1) * rest] = blocks_ref[
                i, lead:, c * LANES : (c + 1) * LANES
            ].astype(f32)

    def turned(r, c):
        return turn_ref[c, pl.ds(r, n_z, stride=rest), :]

    res = jnp.concatenate(
        [turned(r, c) for r in range(dim // width) for c in range(width // LANES)], axis=1
    )
    scale = lax.rsqrt(jnp.sum(ffn * ffn, axis=1, keepdims=True) / dim + EPS)
    stream = res + ffn * scale * post_ref[...]
    scale = lax.rsqrt(jnp.sum(stream * stream, axis=1, keepdims=True) / dim + EPS)
    states = (stream * scale * final_ref[...]).astype(jnp.bfloat16)
    head_ref[...] = states[:, :cut]
    tail_ref[...] = jnp.broadcast_to(states[:, cut:][None], tail_ref.shape)
    digits = turned(dim // width, 0)
    rows = [digits] + [
        pltpu.roll(digits, LANES - DIGITS * i, axis=1) for i in range(1, digit_ref.shape[0] // n_z)
    ]
    digit_ref[...] = jnp.concatenate(rows, axis=0).astype(jnp.bfloat16)


def norm_rows(blocks, post_gain, final_gain, per, cut, copies, toks):
    n_z, rows, width = blocks.shape
    dim = post_gain.shape[0]
    return pl.pallas_call(
        norm_kernel,
        in_specs=[VMEM] * 3,
        out_shape=(
            jax.ShapeDtypeStruct((per, cut), blocks.dtype),
            jax.ShapeDtypeStruct((copies, per, dim - cut), blocks.dtype),
            jax.ShapeDtypeStruct((toks * n_z, LANES), blocks.dtype),
        ),
        scratch_shapes=[pltpu.VMEM((width // LANES, n_z * (rows - per - per // 2), LANES), jnp.float32)],
        compiler_params=pltpu.CompilerParams(vmem_limit_bytes=8 << 20),
        name="norm_rows",
    )(blocks, post_gain[None], final_gain[None])


def sums_kernel(n_z, halves, embed_ref, out_ref, mask_ref, st_ref, acc_ref):
    n_s, held, _ = st_ref.shape
    dim, vocab = embed_ref.shape
    z, x, s = (lax.axis_index(a) for a in ("fsdp", "mp", "sub"))
    first = ((z * lax.axis_size("mp") + x) * n_s + s) * vocab
    for h in range(n_s):
        st_ref[h] = halves[h][...]
    states = st_ref.reshape(n_s * held, st_ref.shape[2])
    acc_ref[...] = dot_f32(states[:, :dim], embed_ref[...], ((1,), (0,)))
    rings_of = [half[:, dim:].astype(jnp.float32) for half in halves]
    token = lax.broadcasted_iota(jnp.int32, rings_of[0].shape, 0) // n_z
    digits = jnp.concatenate(
        [
            jnp.where((token + x) % n_s == 0, rings_of[h], rings_of[n_s - 1 - h])
            for h in range(n_s)
        ],
        axis=0,
    )
    goal = digits[:, 0:1] + 256.0 * digits[:, 1:2] + 65536.0 * digits[:, 2:3]
    goal = goal.astype(jnp.int32) - first
    sums = jnp.zeros((n_s * held, LANES), jnp.float32)
    hits = jnp.zeros((n_s * held, LANES), jnp.float32)
    for v in range(0, vocab, LANES):
        capped = CAP * jnp.tanh(acc_ref[:, v : v + LANES] / CAP)
        ids = lax.broadcasted_iota(jnp.int32, capped.shape, 1) + v
        sums += jnp.exp(capped)
        hits += jnp.where(ids == goal, capped, 0.0)
    rows = [jnp.sum(r.T, axis=0, keepdims=True) for r in (sums, hits)]
    rows.append(digits.T[3:4])
    place = lax.broadcasted_iota(jnp.int32, (1, held), 1)
    core = (place + place // n_z + z + x + s) % n_s
    parts = [
        jnp.where(core == h, row[:, :held], row[:, held:]) for row in rows for h in range(n_s)
    ]
    mask_ref[...] = jnp.concatenate(parts[2 * n_s :], axis=0)
    part = jnp.concatenate(parts[: 2 * n_s], axis=0)
    out_ref[...] = jnp.broadcast_to(part[None], out_ref.shape)


def vocab_sums(halves, embed, n_z, copies):
    n_s, (held, width) = len(halves), halves[0].shape
    dim, vocab = embed.shape

    def kernel(*refs):
        sums_kernel(n_z, refs[:n_s], *refs[n_s:])

    return pl.pallas_call(
        kernel,
        in_specs=[VMEM] * (n_s + 1),
        out_shape=(
            jax.ShapeDtypeStruct((copies, 2 * n_s, held), jnp.float32),
            jax.ShapeDtypeStruct((n_s, held), jnp.float32),
        ),
        scratch_shapes=[
            pltpu.VMEM((n_s, held, width), jnp.bfloat16),
            pltpu.VMEM((n_s * held, vocab), jnp.float32),
        ],
        compiler_params=pltpu.CompilerParams(vmem_limit_bytes=24 << 20),
        cost_estimate=pl.CostEstimate(
            flops=2 * n_s * held * vocab * dim,
            bytes_accessed=2 * (n_s * held + vocab) * dim,
            transcendentals=2 * n_s * held * vocab,
        ),
        name="vocab_sums",
    )(*halves, embed)


def loss_kernel(n_z, packed_ref, mask_ref, token_ref, mean_ref):
    toks = token_ref.shape[0]
    n_s, held = mask_ref.shape
    z, s = lax.axis_index("fsdp"), lax.axis_index("sub")
    packed = jnp.sum(packed_ref[...], axis=0)
    sums, goals, mask = packed[:n_s], packed[n_s:], mask_ref[...]
    losses = mask * (jnp.log(sums) - goals)
    total, count = jnp.sum(losses), jnp.sum(mask)
    whole = jnp.full((1, held), total) / jnp.maximum(jnp.full((1, held), count), 1.0)
    mean_ref[...] = whole[0, :1]
    core = lax.broadcasted_iota(jnp.int32, losses.shape, 0)
    mine = jnp.sum(jnp.where(core == s, losses, 0.0), axis=0, keepdims=True)
    row = lax.broadcasted_iota(jnp.int32, (held, held), 0)
    lane = lax.broadcasted_iota(jnp.int32, (held, held), 1)
    spread = jnp.where((lane == row * n_z + z) & (row < toks), mine, 0.0)
    token_ref[...] = jnp.sum(spread.T, axis=0)[:toks]


def losses_of(packed, mask, n_z, toks):
    return pl.pallas_call(
        functools.partial(loss_kernel, n_z),
        in_specs=[VMEM, VMEM],
        out_shape=(
            jax.ShapeDtypeStruct((toks,), jnp.float32),
            jax.ShapeDtypeStruct((1,), jnp.float32),
        ),
        compiler_params=pltpu.CompilerParams(vmem_limit_bytes=4 << 20),
        name="losses_of",
    )(packed, mask)


def on_device(
    hidden,
    residual,
    down_packed,
    down_scale,
    post_gain,
    final_gain,
    embed_packed,
    embed_scale,
    targets,
    loss_mask,
):
    toks, width = hidden.shape
    n_z, n_x, n_s = (lax.axis_size(a) for a in ("fsdp", "mp", "sub"))
    cols = down_packed.shape[1]
    dim = n_z * cols
    held = n_z * toks
    per_x = held // n_x

    cut = gather_cut(toks, width, n_z)
    head, tail = split_columns(hidden, cut, n_z, width // down_scale.shape[0])
    tail = exchange_ring(tail, "fsdp")
    head_weight, tail_weight = down_weight(down_packed.T, down_scale, cut)
    head, head_weight, tail_weight = lax.optimization_barrier((head, head_weight, tail_weight))
    head = gather_ring(head, "fsdp")
    part = dot_f32(head.reshape(held, cut), head_weight, ((1,), (0,))) + dot_f32(
        tail.reshape(held, width - cut), tail_weight, ((1,), (0,))
    )

    part = jnp.swapaxes(part.reshape(n_z, toks, cols), 0, 1).reshape(n_x, per_x, cols)
    parts = lax.all_to_all(part, "mp", 0, 0, tiled=True)
    parts, residual, targets = lax.optimization_barrier((parts, residual, targets))

    block = pack_rows(targets, loss_mask, parts, residual)
    blocks = gather_ring(block, "fsdp")
    blocks, post_gain, final_gain = lax.optimization_barrier((blocks, post_gain, final_gain))

    cut = gather_cut(per_x, dim, n_x)
    head, tail, digits = norm_rows(blocks, post_gain, final_gain, per_x, cut, n_x, toks)
    tail = exchange_ring(tail, "mp")
    head = gather_ring(head, "mp")
    own = [head.reshape(held, cut), tail.reshape(held, dim - cut), digits]
    own = jnp.concatenate(own, axis=1)
    far = lax.ppermute(own, "sub", [(i, n_s - 1 - i) for i in range(n_s)])
    embed = dequant_embed(embed_packed, embed_scale)
    packed, mask = vocab_sums((own, far), embed.T, n_z, n_x * n_s)

    packed = jnp.sum(lax.all_to_all(packed, ("mp", "sub"), 0, 0, tiled=True), axis=0)
    return losses_of(copy_for_each(packed, "fsdp"), mask, n_z, toks)


def solution(mesh):
    return jax.shard_map(
        on_device,
        mesh=mesh,
        in_specs=(
            P(("groups", "fsdp", "sub"), "mp"),
            P(("groups", "fsdp", "sub"), None),
            P("mp", "fsdp"),
            P("mp", "fsdp"),
            P(),
            P(),
            P(("fsdp", "mp", "sub"), None),
            P(("fsdp", "mp", "sub"), None),
            P(("groups", "fsdp", "sub")),
            P(("groups", "fsdp", "sub")),
        ),
        out_specs=(P(("groups", "fsdp", "sub")), P("groups")),
        check_vma=False,
    )
```
